128 devices in a mesh: scene: 8 (over x, core), slab: 16 (over y, z).
Axes of the slice: x: 4, y: 4, z: 4, core: 2. Of those that a mesh axis runs over, the one named last changes fastest.
Arguments:
- camera_features: bfloat16 [8192, 128, 128], P(('scene', 'slab')), parts along dimension 0, may hold values from -6 to 6
- cell_index: int32 [8192, 128], P('scene'), parts along dimension 0, may hold values from 0 to 127
- owner_device: int32 [8192, 1], P('scene'), parts along dimension 0, may hold values from 0 to 15; in each aligned block of 64 rows (0 to 63, 64 to 127, ...) at most 8 rows name the same one
- owner_tile: int32 [8192], P('scene'), parts along dimension 0, may hold values from 0 to 31
- base_map: bfloat16 [2048, 256, 128], P(('scene', 'slab')), parts along dimension 0, may hold values from -6 to 6
- targets: bfloat16 [2048, 256, 128], P(('scene', 'slab')), parts along dimension 0, may hold values from 0 to 1
- fine_conv: bfloat16 [1152, 128], replicated, may hold values from -0.1875 to 0.1875
- fine_down: bfloat16 [512, 256], replicated, may hold values from -0.25 to 0.25
- middle_conv: bfloat16 [2304, 256], replicated, may hold values from -0.125 to 0.125
- middle_down: bfloat16 [1024, 512], replicated, may hold values from -0.1875 to 0.1875
- coarse_conv: bfloat16 [4608, 512], replicated, may hold values from -0.09375 to 0.09375
- coarse_up: bfloat16 [512, 1024], replicated, may hold values from -0.25 to 0.25
- middle_merge: bfloat16 [2304, 256], replicated, may hold values from -0.125 to 0.125
- middle_up: bfloat16 [256, 512], replicated, may hold values from -0.375 to 0.375
- fine_merge: bfloat16 [1152, 128], replicated, may hold values from -0.1875 to 0.1875
- head_weight: bfloat16 [128, 128], replicated, may hold values from -0.5 to 0.5
Outputs:
- camera_grad: bfloat16 [8192, 128, 128], P(('scene', 'slab')), parts along dimension 0
- row_loss: float32 [2048], P(('scene', 'slab')), parts along dimension 0
- fine_conv_grad: float32 [9216, 128], P(('scene', 'slab')), parts along dimension 0
- fine_down_grad: float32 [4096, 256], P(('scene', 'slab')), parts along dimension 0
- middle_conv_grad: float32 [18432, 256], P(('scene', 'slab')), parts along dimension 0
- middle_down_grad: float32 [8192, 512], P(('scene', 'slab')), parts along dimension 0
- coarse_conv_grad: float32 [36864, 512], P(('scene', 'slab')), parts along dimension 0
- coarse_up_grad: float32 [4096, 1024], P(('scene', 'slab')), parts along dimension 0
- middle_merge_grad: float32 [18432, 256], P(('scene', 'slab')), parts along dimension 0
- middle_up_grad: float32 [2048, 512], P(('scene', 'slab')), parts along dimension 0
- fine_merge_grad: float32 [9216, 128], P(('scene', 'slab')), parts along dimension 0
- head_grad: float32 [1024, 128], P(('scene', 'slab')), parts along dimension 0
The draws below stay inside these ranges and needn't reach their ends.
There are 8 independent parts, one for each index of `scene`. The reference program is written for one: setup_inputs(seed, part) draws one part's arguments, and reference() takes and returns one part's arrays. A program takes and returns all parts, laid end to end along the dimension named above; an argument that names none is the same for every part. Nothing has to cross between parts.
Inputs may be any that keep to these rules, and one draw needn't show every extreme that they name: `owner_device`: of the 64 blocks in each aligned run of 64 rows (the blocks of one index of slab), at most 8 name the same index, a bound that some block reaches of them.
All inputs are finite; a program needn't handle non-finite values.
Results may differ from the reference program's by a relative error of at most 0.017.
Values may be sent and summed in bfloat16 or wider, within the bound.
A program may use at most 192 MiB of HBM per device.

```python
import math
import jax
import jax.numpy as jnp
import numpy as np
from jax import lax

W = 256
BLK_DEV = 64
C0 = 128
C1 = 256
C2 = 512
K = 128
PTS = 128
TILE = 128
CAP = 8
TILES_DEV = 32
ROWS = 256
BLOCKS = 1024
N_SLAB = 16


def plant(array, key, smallest, high):
    longest = array.shape.index(max(array.shape))
    spots = []
    for shift in (0, 1):
        where = [jax.random.randint(jax.random.fold_in(key, axis), (), 0, length) for axis, length in enumerate(array.shape)]
        where[longest] = (where[longest] + shift) % array.shape[longest]
        spots.append(tuple(where))
    return array.at[spots[0]].set(smallest).at[spots[1]].set(high)


def shard_levels(key, dims, cuts, smallest, top_value):
    gain, own = 1.0, jax.random.fold_in(key, 6)
    for axis_at, parts in cuts:
        draws = jnp.exp(jax.random.uniform(jax.random.fold_in(own, axis_at), (parts,), jnp.float32, smallest / len(cuts), top_value / len(cuts)))
        gain = gain * jnp.repeat(draws, dims[axis_at] // parts).reshape([-1 if axis == axis_at else 1 for axis in range(len(dims))])
    return gain


def routed_block(stream_key, own, number, rows, count, top, most, skew):
    sequence = jax.random.permutation(stream_key, count)
    heavy_load, ordinary = load_shares(count, rows * top, most, skew, True), load_shares(count, rows * top, most, skew, False)
    places = jnp.arange(count)

    def named(sizes, rotation):
        used = int((sizes > 0).sum())
        fixed = max(1, used // 4)
        moved = fixed + (places - fixed + rotation * (used - fixed)) % max(1, count - fixed)
        return jnp.zeros((count,), jnp.int32).at[sequence[jnp.where(places < fixed, places, moved)]].set(jnp.asarray(sizes, jnp.int32))

    sizes = jnp.where(number % 4 == 0, named(heavy_load, number // 4), named(ordinary, number - number // 4 - 1))
    mixed = jax.random.permutation(jax.random.fold_in(own, 3), count)
    donor, receiver = mixed[0:count // 2 * 2:2], mixed[1:count // 2 * 2:2]
    room = jnp.minimum(sizes[donor] - 1, most - sizes[receiver]) // 2
    room = jnp.where((donor == sequence[0]) | (receiver == sequence[0]) | (sizes[receiver] == 0), 0, jnp.maximum(room, 0))
    moved = jax.random.randint(jax.random.fold_in(own, 4), (count // 2,), 0, 1 << 20) % (room + 1)
    sizes = sizes.at[donor].add(-moved).at[receiver].add(moved)
    items = jnp.searchsorted(jnp.cumsum(sizes), jnp.arange(rows * top), side="right").astype(jnp.int32)
    grid = items.reshape(top, rows).T
    grid = grid[jax.random.permutation(jax.random.fold_in(own, 1), rows)]
    rotation = jax.random.randint(jax.random.fold_in(own, 2), (rows, 1), 0, top)
    return jnp.take_along_axis(grid, (jnp.arange(top)[None, :] + rotation) % top, axis=1)


def load_shares(amount, total, most, lean, full):
    weights = [(1 << 20) // math.isqrt(standing ** lean) + 1 for standing in range(1, amount + 1)]
    largest = most if full else min(most, max(-(-total // amount), total * weights[0] // sum(weights)))
    least = 1 if total - largest >= amount - 1 else 0
    holding, surplus = [largest] + [least] * (amount - 1), total - largest - least * (amount - 1)
    while surplus > 0:
        movable = [i for i in range(1, amount) if holding[i] < largest] or [i for i in range(1, amount) if holding[i] < most]
        mass, budget = sum([weights[i] for i in movable]), surplus
        for i in movable:
            more = min(most - holding[i], max(1, budget * weights[i] // mass), surplus)
            holding[i] = holding[i] + more
            surplus = surplus - more
    return np.array(holding)


def bell_draw(key, dims, scale, reach, shards=(), kind=jnp.bfloat16):
    values = jax.random.normal(key, dims, jnp.float32) * scale
    if len(shards) > 0:
        values = shard_levels(key, dims, shards, -0.22, 0.18) * values
    return jnp.clip(values, min=-reach, max=reach).astype(kind)


def setup_inputs(seed: int = 0, part: int = 0) -> dict:
    key_list = jax.random.split(jax.random.key(seed), 17)
    own_keys = jax.random.split(jax.random.fold_in(key_list[16], part), 17)
    camera_features = bell_draw(own_keys[0], (BLOCKS, PTS, C0), 1.0, 6.0, ((0, 16),))
    cell_index = plant(jax.random.randint(own_keys[1], (BLOCKS, PTS), 0, TILE), jax.random.fold_in(own_keys[1], 1), 0, TILE - 1).astype(jnp.int32)
    owner_device_keys = jax.random.split(jax.random.fold_in(own_keys[2], 1), BLOCKS // BLK_DEV)
    owner_device_turns = jax.random.permutation(jax.random.fold_in(own_keys[2], 3), BLOCKS // BLK_DEV)
    owner_device = jax.vmap(lambda own, number: routed_block(jax.random.fold_in(own_keys[2], 2), own, number, BLK_DEV, N_SLAB, 1, CAP, 2))(owner_device_keys, owner_device_turns).reshape((BLOCKS, 1))
    owner_tile = plant(jax.random.randint(own_keys[3], (BLOCKS,), 0, TILES_DEV), jax.random.fold_in(own_keys[3], 1), 0, TILES_DEV - 1).astype(jnp.int32)
    base_map = bell_draw(own_keys[4], (ROWS, W, C0), 1.0, 6.0, ((0, 16),))
    targets = jnp.clip(1.0 * jax.random.uniform(own_keys[5], (ROWS, W, K), jnp.float32) ** shard_levels(own_keys[5], (ROWS, W, K), ((0, 16),), -0.2, 0.2), 0.0, 1.0).astype(jnp.bfloat16)
    fine_conv = bell_draw(key_list[6], (9 * C0, C0), (9 * C0) ** -0.5, 0.1875)
    fine_down = bell_draw(key_list[7], (4 * C0, C1), (4 * C0) ** -0.5, 0.25)
    middle_conv = bell_draw(key_list[8], (9 * C1, C1), (9 * C1) ** -0.5, 0.125)
    middle_down = bell_draw(key_list[9], (4 * C1, C2), (4 * C1) ** -0.5, 0.1875)
    coarse_conv = bell_draw(key_list[10], (9 * C2, C2), (9 * C2) ** -0.5, 0.09375)
    coarse_up = bell_draw(key_list[11], (C2, 4 * C1), C2 ** -0.5, 0.25)
    middle_merge = bell_draw(key_list[12], (9 * C1, C1), (9 * C1) ** -0.5, 0.125)
    middle_up = bell_draw(key_list[13], (C1, 4 * C0), C1 ** -0.5, 0.375)
    fine_merge = bell_draw(key_list[14], (9 * C0, C0), (9 * C0) ** -0.5, 0.1875)
    head_weight = bell_draw(key_list[15], (C0, K), C0 ** -0.5, 0.5)
    return {"camera_features": camera_features, "cell_index": cell_index, "owner_device": owner_device, "owner_tile": owner_tile, "base_map": base_map, "targets": targets, "fine_conv": fine_conv, "fine_down": fine_down, "middle_conv": middle_conv, "middle_down": middle_down, "coarse_conv": coarse_conv, "coarse_up": coarse_up, "middle_merge": middle_merge, "middle_up": middle_up, "fine_merge": fine_merge, "head_weight": head_weight}


loss_weight = 0.0625


def window_taps(padded):
    height = padded.shape[0] - 2
    across = padded.shape[1]
    framed = jnp.pad(padded, ((0, 0), (1, 1), (0, 0)))
    pieces = [framed[1 + row_step:1 + row_step + height, 1 + column_step:1 + column_step + across]
              for row_step in (-1, 0, 1) for column_step in (-1, 0, 1)]
    return jnp.concatenate(pieces, axis=-1).reshape(height * across, -1)


def flipped(weight):
    inward = weight.shape[0] // 9
    return weight.reshape(9, inward, -1)[::-1].transpose(0, 2, 1).reshape(-1, inward)


def fold_pairs(field):
    height, across, channels = field.shape
    return field.reshape(height // 2, 2, across // 2, 2, channels).transpose(0, 2, 1, 3, 4).reshape(
        (height // 2) * (across // 2), 4 * channels)


def unfold_pairs(matrix, height, across):
    channels = matrix.shape[1] // 4
    return matrix.reshape(height, across, 2, 2, channels).transpose(0, 2, 1, 3, 4).reshape(
        2 * height, 2 * across, channels)


def silu_slope(signal):
    logistic = jax.nn.sigmoid(signal)
    return logistic * (1.0 + signal * (1.0 - logistic))


def outer(former, latter):
    return lax.dot_general(former, latter, (((0,), (0,)), ((), ())), preferred_element_type=jnp.float32)


def backward(former, latter):
    return lax.dot_general(former, latter, (((1,), (1,)), ((), ())), preferred_element_type=jnp.float32)


def conv_whole(field, weight):
    padded = jnp.pad(field, ((1, 1), (0, 0), (0, 0)))
    taps = window_taps(padded)
    result = jnp.dot(taps, weight, preferred_element_type=jnp.float32)
    return result.reshape(field.shape[0], field.shape[1], -1), taps


def reference(camera_features, cell_index, owner_device, owner_tile, base_map, targets, fine_conv, fine_down,
              middle_conv, middle_down, coarse_conv, coarse_up, middle_merge, middle_up, fine_merge, head_weight):
    single = jnp.float32
    bfloat = jnp.bfloat16
    cell_onehot = (cell_index[:, :, None] == jnp.arange(TILE, dtype=jnp.int32)[None, None, :]).astype(single)
    deposits = jnp.einsum("bpt,bpc->btc", cell_onehot, camera_features.astype(single)).astype(bfloat)
    tile_number = (owner_device[:, 0] * TILES_DEV + owner_tile).astype(jnp.int32)
    canvas = jax.ops.segment_sum(deposits.astype(single).reshape(BLOCKS, -1), tile_number,
                                 num_segments=N_SLAB * TILES_DEV)
    level_zero = (base_map.astype(single) + canvas.reshape(ROWS, W, C0)).astype(bfloat)

    half_height, half_across = ROWS // 2, W // 2
    quarter_height, quarter_across = ROWS // 4, W // 4

    pre_fine, taps_fine = conv_whole(level_zero, fine_conv)
    hidden_fine = jax.nn.silu(pre_fine).astype(bfloat)
    quarter_fine = fold_pairs(hidden_fine)
    level_one = jnp.dot(quarter_fine, fine_down, preferred_element_type=single).astype(bfloat).reshape(
        half_height, half_across, C1)
    pre_middle, taps_middle = conv_whole(level_one, middle_conv)
    hidden_middle = jax.nn.silu(pre_middle).astype(bfloat)
    quarter_middle = fold_pairs(hidden_middle)
    level_two = jnp.dot(quarter_middle, middle_down, preferred_element_type=single).astype(bfloat).reshape(
        quarter_height, quarter_across, C2)
    pre_coarse, taps_coarse = conv_whole(level_two, coarse_conv)
    hidden_coarse = jax.nn.silu(pre_coarse).astype(bfloat)
    lifted = jnp.dot(hidden_coarse.reshape(-1, C2), coarse_up, preferred_element_type=single)
    joined_middle = (unfold_pairs(lifted, quarter_height, quarter_across)
                     + hidden_middle.astype(single)).astype(bfloat)
    pre_merge, taps_merge = conv_whole(joined_middle, middle_merge)
    out_middle = jax.nn.silu(pre_merge).astype(bfloat)
    raised = jnp.dot(out_middle.reshape(-1, C1), middle_up, preferred_element_type=single)
    joined_fine = (unfold_pairs(raised, half_height, half_across) + hidden_fine.astype(single)).astype(bfloat)
    pre_top, taps_top = conv_whole(joined_fine, fine_merge)
    out_fine = jax.nn.silu(pre_top).astype(bfloat)
    logits = jnp.dot(out_fine.reshape(-1, C0), head_weight, preferred_element_type=single)
    labels = targets.reshape(-1, K).astype(single)
    penalty = jax.nn.softplus(logits) - labels * logits
    row_loss = jnp.sum(penalty.reshape(ROWS, -1), axis=1) / (W * K)

    slope_logits = ((jax.nn.sigmoid(logits) - labels) * loss_weight).astype(bfloat)
    head_grad = outer(out_fine.reshape(-1, C0), slope_logits)
    back_top = (backward(slope_logits, head_weight) * silu_slope(pre_top.reshape(-1, C0))).astype(bfloat)
    fine_merge_grad = outer(taps_top, back_top)
    gradient_fine, _ = conv_whole(back_top.reshape(ROWS, W, C0), flipped(fine_merge))
    joined_fine_grad = gradient_fine.astype(bfloat)
    folded_fine_grad = fold_pairs(joined_fine_grad)
    middle_up_grad = outer(out_middle.reshape(-1, C1), folded_fine_grad)
    back_merge = (backward(folded_fine_grad, middle_up) * silu_slope(pre_merge.reshape(-1, C1))).astype(bfloat)
    middle_merge_grad = outer(taps_merge, back_merge)
    gradient_middle, _ = conv_whole(back_merge.reshape(half_height, half_across, C1), flipped(middle_merge))
    joined_middle_grad = gradient_middle.astype(bfloat)
    folded_middle_grad = fold_pairs(joined_middle_grad)
    coarse_up_grad = outer(hidden_coarse.reshape(-1, C2), folded_middle_grad)
    back_coarse = (backward(folded_middle_grad, coarse_up) * silu_slope(pre_coarse.reshape(-1, C2))).astype(bfloat)
    coarse_conv_grad = outer(taps_coarse, back_coarse)
    gradient_coarse, _ = conv_whole(back_coarse.reshape(quarter_height, quarter_across, C2), flipped(coarse_conv))
    level_two_grad = gradient_coarse.astype(bfloat)
    middle_down_grad = outer(quarter_middle, level_two_grad.reshape(-1, C2))
    spread = unfold_pairs(backward(level_two_grad.reshape(-1, C2), middle_down), quarter_height, quarter_across)
    back_middle = ((joined_middle_grad.astype(single) + spread) * silu_slope(pre_middle)).astype(bfloat)
    middle_conv_grad = outer(taps_middle, back_middle.reshape(-1, C1))
    gradient_one, _ = conv_whole(back_middle, flipped(middle_conv))
    level_one_grad = gradient_one.astype(bfloat)
    fine_down_grad = outer(quarter_fine, level_one_grad.reshape(-1, C1))
    spread_fine = unfold_pairs(backward(level_one_grad.reshape(-1, C1), fine_down), half_height, half_across)
    back_fine = ((joined_fine_grad.astype(single) + spread_fine) * silu_slope(pre_fine)).astype(bfloat)
    fine_conv_grad = outer(taps_fine, back_fine.reshape(-1, C0))
    gradient_zero, _ = conv_whole(back_fine, flipped(fine_conv))
    level_zero_grad = gradient_zero.astype(bfloat)

    tiles_grad = level_zero_grad.reshape(N_SLAB * TILES_DEV, TILE, C0)
    picked = tiles_grad[tile_number]
    camera_grad = jnp.einsum("bpt,btc->bpc", cell_onehot, picked.astype(single)).astype(bfloat)
    return (camera_grad, row_loss, fine_conv_grad, fine_down_grad, middle_conv_grad, middle_down_grad,
            coarse_conv_grad, coarse_up_grad, middle_merge_grad, middle_up_grad, fine_merge_grad, head_grad)
```

```python
import jax
import jax.numpy as jnp
from jax import lax
from jax.sharding import PartitionSpec as P


BLK_DEV = 64
C1 = 256
C2 = 512
K = 128
TILE = 128
CAP = 8


loss_weight = 0.0625


def extended(block, sides, width):
    for axis, dim in sides:
        count = lax.axis_size(axis)
        forward = [(i, i + 1) for i in range(count - 1)]
        backward = [(target, source) for source, target in forward]
        low = lax.ppermute(
            lax.slice_in_dim(block, block.shape[dim] - width, None, axis=dim), axis, forward
        )
        high = lax.ppermute(lax.slice_in_dim(block, 0, width, axis=dim), axis, backward)
        block = jnp.concatenate([low, block, high], axis=dim)
    return block


def as_lines(block, width):
    rows, columns = block.shape[-2], block.shape[-1]
    if columns >= width:
        parts = [block[..., at : at + width] for at in range(0, columns, width)]
        return jnp.concatenate(parts, axis=-2)
    step = rows * columns // width
    parts = [block[..., at : at + step, :] for at in range(0, rows, step)]
    return jnp.concatenate(parts, axis=-1)


def from_lines(lines, rows, columns):
    width = lines.shape[1]
    if columns >= width:
        return jnp.concatenate([lines[at : at + rows] for at in range(0, lines.shape[0], rows)], 1)
    return jnp.concatenate([lines[:, at : at + columns] for at in range(0, width, columns)], 0)


def sum_packed(arrays, axis, width=512):
    size = lax.axis_size(axis)
    shapes = [(array.shape[0] // size, array.shape[1]) for array in arrays]
    pieces = [as_lines(a.reshape(size, *shape), width) for a, shape in zip(arrays, shapes)]
    total = sum(piece.shape[1] for piece in pieces)
    spare = -total % 16
    if spare:
        pieces.append(jnp.zeros((size, spare, width), arrays[0].dtype))
    lines = lax.optimization_barrier(jnp.concatenate(pieces, axis=1).reshape(-1, width))
    summed = lax.psum_scatter(lines, axis, scatter_dimension=0, tiled=True)
    summed = lax.optimization_barrier(summed)
    at, outs = 0, []
    for rows, columns in shapes:
        count = rows * columns // width
        outs.append(from_lines(summed[at : at + count], rows, columns).astype(jnp.float32))
        at += count
    return outs


def window_taps(padded):
    height = padded.shape[0] - 2
    across = padded.shape[1]
    framed = jnp.pad(padded, ((0, 0), (1, 1), (0, 0)))
    pieces = [
        framed[1 + row_step : 1 + row_step + height, 1 + column_step : 1 + column_step + across]
        for row_step in (-1, 0, 1)
        for column_step in (-1, 0, 1)
    ]
    return jnp.concatenate(pieces, axis=-1).reshape(height * across, -1)


def flipped(weight):
    inward = weight.shape[0] // 9
    return weight.reshape(9, inward, -1)[::-1].transpose(0, 2, 1).reshape(-1, inward)


def fold_pairs(field):
    height, across, channels = field.shape
    return (
        field.reshape(height // 2, 2, across // 2, 2, channels)
        .transpose(0, 2, 1, 3, 4)
        .reshape(height // 2 * (across // 2), 4 * channels)
    )


def unfold_pairs(matrix, height, across):
    channels = matrix.shape[1] // 4
    return (
        matrix.reshape(height, across, 2, 2, channels)
        .transpose(0, 2, 1, 3, 4)
        .reshape(2 * height, 2 * across, channels)
    )


def silu_slope(signal):
    logistic = jax.nn.sigmoid(signal)
    return logistic * (1.0 + signal * (1.0 - logistic))


def outer(former, latter):
    return lax.dot_general(
        former, latter, (((0,), (0,)), ((), ())), preferred_element_type=jnp.float32
    )


def backward(former, latter):
    return lax.dot_general(
        former, latter, (((1,), (1,)), ((), ())), preferred_element_type=jnp.float32
    )


def rim_conv(field, weight):
    height, across = (field.shape[0], field.shape[1])
    padded = extended(field, (("slab", 0),), 1)
    taps = window_taps(padded)
    result = jnp.dot(taps, weight, preferred_element_type=jnp.float32)
    return (result.reshape(height, across, -1), taps)


def body(
    camera_features,
    cell_index,
    owner_device,
    owner_tile,
    base_map,
    targets,
    fine_conv,
    fine_down,
    middle_conv,
    middle_down,
    coarse_conv,
    coarse_up,
    middle_merge,
    middle_up,
    fine_merge,
    head_weight,
):
    single = jnp.float32
    bfloat = jnp.bfloat16
    device = lax.axis_index("slab")
    devices = lax.axis_size("slab")
    height, across, channels = base_map.shape
    slot_count = devices * CAP
    tile_count = height * across // TILE
    owners = owner_device[:, 0]
    everyone = owners.shape[0]
    choose = (owners[:, None] == jnp.arange(devices, dtype=jnp.int32)[None, :]).astype(jnp.int32)
    grouped = choose.reshape(devices, BLK_DEV, devices)
    earlier = (jnp.cumsum(grouped, axis=1) - grouped).reshape(everyone, devices)
    ranking = jnp.sum(earlier * choose, axis=1)
    sources = jnp.arange(everyone, dtype=jnp.int32) // BLK_DEV
    slot_number = owners * CAP + ranking
    local_slot = lax.dynamic_slice_in_dim(slot_number, device * BLK_DEV, BLK_DEV)
    slot_range = jnp.arange(slot_count, dtype=jnp.int32)
    send_map = (local_slot[None, :] == slot_range[:, None]).astype(bfloat)
    arrival = sources * CAP + ranking
    receive_map = ((arrival[None, :] == slot_range[:, None]) & (owners[None, :] == device)).astype(
        jnp.int32
    )
    tile_onehot = (owner_tile[:, None] == jnp.arange(tile_count, dtype=jnp.int32)[None, :]).astype(
        jnp.int32
    )
    placement = jnp.einsum("bt,sb->ts", tile_onehot, receive_map).astype(bfloat)
    cell_range = jnp.arange(TILE, dtype=jnp.int32)
    local_cells = lax.dynamic_slice_in_dim(cell_index, device * BLK_DEV, BLK_DEV)
    cell_onehot = (local_cells[:, :, None] == cell_range[None, None, :]).astype(bfloat)
    payload = (
        jnp.einsum("bpt,bpc->btc", cell_onehot, camera_features, preferred_element_type=single)
        .astype(bfloat)
        .reshape(BLK_DEV, -1)
    )
    outgoing = (
        jnp.dot(send_map, payload, preferred_element_type=single)
        .astype(bfloat)
        .reshape(devices, CAP, -1)
    )
    incoming = lax.all_to_all(outgoing, "slab", split_axis=0, concat_axis=0, tiled=True).reshape(
        slot_count, -1
    )
    canvas = jnp.dot(placement, incoming, preferred_element_type=single).reshape(
        height, across, channels
    )
    level_zero = (base_map.astype(single) + canvas).astype(bfloat)
    half_height, half_across = (height // 2, across // 2)
    quarter_height, quarter_across = (height // 4, across // 4)
    pre_fine, taps_fine = rim_conv(level_zero, fine_conv)
    hidden_fine = jax.nn.silu(pre_fine).astype(bfloat)
    quarter_fine = fold_pairs(hidden_fine)
    level_one = (
        jnp.dot(quarter_fine, fine_down, preferred_element_type=single)
        .astype(bfloat)
        .reshape(half_height, half_across, C1)
    )
    pre_middle, taps_middle = rim_conv(level_one, middle_conv)
    hidden_middle = jax.nn.silu(pre_middle).astype(bfloat)
    quarter_middle = fold_pairs(hidden_middle)
    level_two = (
        jnp.dot(quarter_middle, middle_down, preferred_element_type=single)
        .astype(bfloat)
        .reshape(quarter_height, quarter_across, C2)
    )
    pre_coarse, taps_coarse = rim_conv(level_two, coarse_conv)
    hidden_coarse = jax.nn.silu(pre_coarse).astype(bfloat)
    lifted = jnp.dot(hidden_coarse.reshape(-1, C2), coarse_up, preferred_element_type=single)
    joined_middle = (
        unfold_pairs(lifted, quarter_height, quarter_across) + hidden_middle.astype(single)
    ).astype(bfloat)
    pre_merge, taps_merge = rim_conv(joined_middle, middle_merge)
    out_middle = jax.nn.silu(pre_merge).astype(bfloat)
    raised = jnp.dot(out_middle.reshape(-1, C1), middle_up, preferred_element_type=single)
    joined_fine = (
        unfold_pairs(raised, half_height, half_across) + hidden_fine.astype(single)
    ).astype(bfloat)
    pre_top, taps_top = rim_conv(joined_fine, fine_merge)
    out_fine = jax.nn.silu(pre_top).astype(bfloat)
    logits = jnp.dot(out_fine.reshape(-1, channels), head_weight, preferred_element_type=single)
    labels = targets.reshape(-1, K).astype(single)
    penalty = jax.nn.softplus(logits) - labels * logits
    row_loss = jnp.sum(penalty.reshape(height, -1), axis=1) / (across * K)
    slope_logits = ((jax.nn.sigmoid(logits) - labels) * loss_weight).astype(bfloat)
    head_grad = outer(out_fine.reshape(-1, channels), slope_logits)
    back_top = (
        backward(slope_logits, head_weight) * silu_slope(pre_top.reshape(-1, channels))
    ).astype(bfloat)
    fine_merge_grad = outer(taps_top, back_top)
    gradient_fine, _ = rim_conv(back_top.reshape(height, across, channels), flipped(fine_merge))
    joined_fine_grad = gradient_fine.astype(bfloat)
    folded_fine_grad = fold_pairs(joined_fine_grad)
    middle_up_grad = outer(out_middle.reshape(-1, C1), folded_fine_grad)
    back_merge = (
        backward(folded_fine_grad, middle_up) * silu_slope(pre_merge.reshape(-1, C1))
    ).astype(bfloat)
    middle_merge_grad = outer(taps_merge, back_merge)
    gradient_middle, _ = rim_conv(
        back_merge.reshape(half_height, half_across, C1), flipped(middle_merge)
    )
    joined_middle_grad = gradient_middle.astype(bfloat)
    folded_middle_grad = fold_pairs(joined_middle_grad)
    coarse_up_grad = outer(hidden_coarse.reshape(-1, C2), folded_middle_grad)
    back_coarse = (
        backward(folded_middle_grad, coarse_up) * silu_slope(pre_coarse.reshape(-1, C2))
    ).astype(bfloat)
    coarse_conv_grad = outer(taps_coarse, back_coarse)
    (
        coarse_conv_sum,
        coarse_up_sum,
        middle_merge_sum,
        middle_up_sum,
        fine_merge_sum,
        head_sum,
    ) = sum_packed(
        [
            g.astype(bfloat)
            for g in (
                coarse_conv_grad,
                coarse_up_grad,
                middle_merge_grad,
                middle_up_grad,
                fine_merge_grad,
                head_grad,
            )
        ],
        "slab",
    )
    gradient_coarse, _ = rim_conv(
        back_coarse.reshape(quarter_height, quarter_across, C2), flipped(coarse_conv)
    )
    level_two_grad = gradient_coarse.astype(bfloat)
    middle_down_grad = outer(quarter_middle, level_two_grad.reshape(-1, C2))
    spread = unfold_pairs(
        backward(level_two_grad.reshape(-1, C2), middle_down), quarter_height, quarter_across
    )
    back_middle = ((joined_middle_grad.astype(single) + spread) * silu_slope(pre_middle)).astype(
        bfloat
    )
    middle_conv_grad = outer(taps_middle, back_middle.reshape(-1, C1))
    gradient_one, _ = rim_conv(back_middle, flipped(middle_conv))
    level_one_grad = gradient_one.astype(bfloat)
    fine_down_grad = outer(quarter_fine, level_one_grad.reshape(-1, C1))
    spread_fine = unfold_pairs(
        backward(level_one_grad.reshape(-1, C1), fine_down), half_height, half_across
    )
    back_fine = ((joined_fine_grad.astype(single) + spread_fine) * silu_slope(pre_fine)).astype(
        bfloat
    )
    fine_conv_grad = outer(taps_fine, back_fine.reshape(-1, channels))
    middle_down_sum, middle_conv_sum, fine_down_sum, fine_conv_sum = sum_packed(
        [
            g.astype(bfloat)
            for g in (middle_down_grad, middle_conv_grad, fine_down_grad, fine_conv_grad)
        ],
        "slab",
    )
    gradient_zero, _ = rim_conv(back_fine, flipped(fine_conv))
    level_zero_grad = gradient_zero.astype(bfloat)
    tiles_grad = level_zero_grad.reshape(tile_count, -1)
    slot_grad = jnp.einsum(
        "ts,tl->sl", placement, tiles_grad, preferred_element_type=single
    ).astype(bfloat)
    returned = lax.all_to_all(
        slot_grad.reshape(devices, CAP, -1), "slab", split_axis=0, concat_axis=0, tiled=True
    ).reshape(slot_count, -1)
    own_blocks = jnp.einsum("sb,sl->bl", send_map, returned, preferred_element_type=single).astype(
        bfloat
    )
    camera_grad = jnp.einsum(
        "bpt,btc->bpc",
        cell_onehot,
        own_blocks.reshape(BLK_DEV, TILE, channels),
        preferred_element_type=single,
    ).astype(bfloat)
    return (
        camera_grad,
        row_loss,
        fine_conv_sum,
        fine_down_sum,
        middle_conv_sum,
        middle_down_sum,
        coarse_conv_sum,
        coarse_up_sum,
        middle_merge_sum,
        middle_up_sum,
        fine_merge_sum,
        head_sum,
    )


def solution(mesh):
    return jax.shard_map(
        body,
        mesh=mesh,
        in_specs=(
            P(("scene", "slab"), None, None),
            P("scene", None),
            P("scene", None),
            P("scene"),
            P(("scene", "slab"), None, None),
            P(("scene", "slab"), None, None),
            P(),
            P(),
            P(),
            P(),
            P(),
            P(),
            P(),
            P(),
            P(),
            P(),
        ),
        out_specs=(
            P(("scene", "slab"), None, None),
            P(("scene", "slab")),
            P(("scene", "slab"), None),
            P(("scene", "slab"), None),
            P(("scene", "slab"), None),
            P(("scene", "slab"), None),
            P(("scene", "slab"), None),
            P(("scene", "slab"), None),
            P(("scene", "slab"), None),
            P(("scene", "slab"), None),
            P(("scene", "slab"), None),
            P(("scene", "slab"), None),
        ),
        check_vma=False,
    )
```

```python
import functools

import jax
import jax.numpy as jnp
from jax import lax
from jax.experimental import pallas as pl
from jax.experimental.pallas import tpu as pltpu
from jax.sharding import PartitionSpec as P

BLK_DEV = 64
C1 = 256
C2 = 512
K = 128
TILE = 128
CAP = 8
MESH = pl.DeviceIdType.MESH


loss_weight = 0.0625


def flipped(weight):
    inward = weight.shape[0] // 9
    return weight.reshape(9, inward, -1)[::-1].transpose(0, 2, 1).reshape(-1, inward)


def silu_slope(signal):
    logistic = jax.nn.sigmoid(signal)
    return logistic * (1.0 + signal * (1.0 - logistic))


def outer(former, latter):
    return lax.dot_general(
        former, latter, (((0,), (0,)), ((), ())), preferred_element_type=jnp.float32
    )


def backward(former, latter):
    return lax.dot_general(
        former, latter, (((1,), (1,)), ((), ())), preferred_element_type=jnp.float32
    )


def lower_rows(block):
    moved = pltpu.roll(block.astype(jnp.float32), 1, 0)
    place = lax.broadcasted_iota(jnp.int32, moved.shape, 0)
    return jnp.where(place == 0, 0.0, moved).astype(block.dtype)


def upper_rows(block):
    length = block.shape[0]
    moved = pltpu.roll(block.astype(jnp.float32), length - 1, 0)
    place = lax.broadcasted_iota(jnp.int32, moved.shape, 0)
    return jnp.where(place == length - 1, 0.0, moved).astype(block.dtype)


def shifted_pair(row):
    span = 64
    blocks = [row[at : at + span] for at in range(0, row.shape[0], span)]
    if len(blocks) == 1:
        return lower_rows(row), upper_rows(row)
    if len(blocks) == 2:
        left = [lower_rows(blocks[1]), blocks[0]]
        right = [blocks[1], upper_rows(blocks[0])]
    else:
        left = [lower_rows(blocks[3]), blocks[2], blocks[0], blocks[1]]
        right = [blocks[2], blocks[3], blocks[1], upper_rows(blocks[0])]
    return jnp.concatenate(left, axis=0), jnp.concatenate(right, axis=0)


def window(start, size):
    if isinstance(start, int):
        return pl.ds(start, size)
    return pl.ds(pl.multiple_of(start, size if size < 64 else 64), size)


def put_row(field, at, row):
    span, channels = row.shape
    left, right = shifted_pair(row)
    rows = window(at * span, span)
    field[rows, 0:channels] = left
    field[rows, channels : 2 * channels] = row
    field[rows, 2 * channels : 3 * channels] = right


def tap_rows(field, first, count, span):
    return jnp.concatenate(
        [field[window((first + step) * span, count * span), :] for step in range(3)], axis=1
    )


def times(former, latter):
    return jnp.dot(former, latter, preferred_element_type=jnp.float32)


def unet_kernel(*refs):
    (
        zero_ref, labels_ref, fine_conv, fine_down, middle_conv, middle_down, coarse_conv,
        coarse_up, middle_merge, middle_up, fine_merge, head, flip_fine, flip_middle,
        flip_coarse, flip_merge, flip_top,
        zero_grad, loss_ref, g_fine, g_fine_down, g_middle, g_middle_down, g_coarse,
        g_coarse_up, g_merge, g_up, g_top, g_head,
        field_zero, field_top, field_fine, field_one, field_merge, field_middle, field_two,
        field_coarse, pre_fine, hid_fine, pre_middle, hid_middle, pre_coarse, hid_coarse,
        pre_merge, out_middle, grad_fine, grad_middle, grad_one, sum_fine, sum_middle, sum_head,
        edges_fine, edges_middle, edges_coarse, halo_fine, halo_middle, halo_coarse,
        send_sem, receive_sem,
    ) = refs
    bfloat, single = jnp.bfloat16, jnp.float32
    slab = lax.axis_index("slab")
    last = lax.axis_size("slab") - 1
    barrier = pltpu.get_barrier_semaphore()

    for step in (1, last):
        pl.semaphore_signal(
            barrier,
            inc=1,
            device_id={"slab": lax.rem(slab + step, last + 1)},
            device_id_type=MESH,
        )
    pl.semaphore_wait(barrier, 2)

    def edge_copy(source, halo, exchange, slot, way):
        return pltpu.make_async_remote_copy(
            src_ref=source,
            dst_ref=halo.at[slot, way],
            send_sem=send_sem.at[exchange, way],
            recv_sem=receive_sem.at[exchange, way],
            device_id={"slab": slab + (1 if way == 0 else -1)},
            device_id_type=MESH,
        )

    started = []

    def send_edges(top, bottom, halo, exchange, slot):
        started.append((top, bottom, halo, exchange, slot))

        @pl.when(slab < last)
        def _():
            edge_copy(bottom, halo, exchange, slot, 0).start()

        @pl.when(slab > 0)
        def _():
            edge_copy(top, halo, exchange, slot, 1).start()

    def take_edges(field, height):
        top, bottom, halo, exchange, slot = started[-1]

        @pl.when(slab > 0)
        def _():
            edge_copy(bottom, halo, exchange, slot, 0).wait_recv()

        @pl.when(slab == 0)
        def _():
            halo[slot, 0] = jnp.zeros(halo.shape[2:], halo.dtype)

        @pl.when(slab < last)
        def _():
            edge_copy(top, halo, exchange, slot, 1).wait_recv()

        @pl.when(slab == last)
        def _():
            halo[slot, 1] = jnp.zeros(halo.shape[2:], halo.dtype)

        put_row(field, 0, halo[slot, 0])
        put_row(field, height + 1, halo[slot, 1])

    def each(first, bound, body):
        def step(index, carry):
            body(index)
            return carry

        lax.fori_loop(first, bound, step, 0)

    def fine_rows(handle, inner, outer_):
        if inner:
            each(1, 7, handle)
        if outer_:
            each(0, 2, lambda index: handle(index * 7))

    def middle_rows(handle, inner, outer_):
        if inner:
            each(1, 3, handle)
        if outer_:
            each(0, 2, lambda index: handle(index * 3))

    quads = [(0, 0), (0, 1), (1, 0), (1, 1)]

    send_edges(zero_ref.at[0], zero_ref.at[15], halo_fine, 0, 0)
    each(0, 16, lambda row: put_row(field_zero, row + 1, zero_ref[row]))

    def fine_step(at):
        pre = times(tap_rows(field_zero, 2 * at, 2, 256), fine_conv[...])
        rows = window(at * 128, 128)
        for k in range(4):
            part = pre[k * 128 : (k + 1) * 128]
            pre_fine[rows, k * 128 : (k + 1) * 128] = part
            hid_fine[rows, k * 128 : (k + 1) * 128] = jax.nn.silu(part).astype(bfloat)

    fine_rows(fine_step, True, False)
    take_edges(field_zero, 16)
    fine_rows(fine_step, False, True)

    def one_step(at):
        value = times(hid_fine[window(at * 256, 256), :], fine_down[...]).astype(bfloat)
        for k in range(2):
            put_row(field_one, 2 * at + k + 1, value[k * 128 : (k + 1) * 128])

    def middle_edges(field, slot):
        edges_middle[slot, 0] = field[pl.ds(128, 128), 256:512]
        edges_middle[slot, 1] = field[pl.ds(8 * 128, 128), 256:512]

    middle_rows(one_step, False, True)
    middle_edges(field_one, 0)
    send_edges(edges_middle.at[0, 0], edges_middle.at[0, 1], halo_middle, 1, 0)
    middle_rows(one_step, True, False)

    def middle_step(at):
        pre = times(tap_rows(field_one, 2 * at, 2, 128), middle_conv[...])
        rows = window(at * 64, 64)
        for k in range(4):
            part = pre[k * 64 : (k + 1) * 64]
            pre_middle[rows, k * 256 : (k + 1) * 256] = part
            hid_middle[rows, k * 256 : (k + 1) * 256] = jax.nn.silu(part).astype(bfloat)

    middle_rows(middle_step, True, False)
    take_edges(field_one, 8)
    middle_rows(middle_step, False, True)

    def spread_coarse(field, value, slot, exchange):
        for row in range(4):
            put_row(field, row + 1, value[row * 64 : (row + 1) * 64])
        edges_coarse[slot, 0] = value[0:64]
        edges_coarse[slot, 1] = value[192:256]
        send_edges(edges_coarse.at[slot, 0], edges_coarse.at[slot, 1], halo_coarse, exchange, slot)

    def coarse_part(field, weight, step):
        return times(
            field[window(step * 64, 256), :], weight[window(step * 1536, 1536), :]
        )

    value = times(hid_middle[...], middle_down[...]).astype(bfloat)
    spread_coarse(field_two, value, 0, 2)
    pre_coarse[...] = coarse_part(field_two, coarse_conv, 1)
    take_edges(field_two, 4)

    def coarse_step(index):
        pre_coarse[...] += coarse_part(field_two, coarse_conv, 2 * index)

    each(0, 2, coarse_step)
    hid_coarse[...] = jax.nn.silu(pre_coarse[...]).astype(bfloat)

    def join_middle(at):
        rows = window(at * 64, 64)
        total = times(hid_coarse[rows, :], coarse_up[...]) + hid_middle[rows, :].astype(single)
        total = total.astype(bfloat)
        for i in range(2):
            row = jnp.concatenate(
                [total[:, (2 * i + j) * 256 : (2 * i + j + 1) * 256] for j in range(2)], axis=0
            )
            put_row(field_merge, 2 * at + i + 1, row)

    middle_rows(join_middle, False, True)
    middle_edges(field_merge, 1)
    send_edges(edges_middle.at[1, 0], edges_middle.at[1, 1], halo_middle, 3, 1)
    middle_rows(join_middle, True, False)

    def merge_step(at):
        pre = times(tap_rows(field_merge, 2 * at, 2, 128), middle_merge[...])
        rows = window(at * 256, 256)
        pre_merge[rows, :] = pre
        out_middle[rows, :] = jax.nn.silu(pre).astype(bfloat)

    middle_rows(merge_step, True, False)
    take_edges(field_merge, 8)
    middle_rows(merge_step, False, True)

    def join_fine(at):
        rows = window(at * 128, 128)
        total = times(out_middle[rows, :], middle_up[...]) + hid_fine[rows, :].astype(single)
        total = total.astype(bfloat)
        for i in range(2):
            row = jnp.concatenate(
                [total[:, (2 * i + j) * 128 : (2 * i + j + 1) * 128] for j in range(2)], axis=0
            )
            put_row(field_top, 2 * at + i + 1, row)

    def fine_edges(field, slot):
        edges_fine[slot, 0] = field[pl.ds(256, 256), 128:256]
        edges_fine[slot, 1] = field[pl.ds(16 * 256, 256), 128:256]

    fine_rows(join_fine, False, True)
    fine_edges(field_top, 0)
    send_edges(edges_fine.at[0, 0], edges_fine.at[0, 1], halo_fine, 4, 1)
    fine_rows(join_fine, True, False)
    sum_head[...] = jnp.zeros_like(sum_head)

    def top_step(at):
        pre = times(tap_rows(field_top, 2 * at, 2, 256), fine_merge[...])
        logistic = jax.nn.sigmoid(pre)
        out_fine = (pre * logistic).astype(bfloat)
        logits = times(out_fine, head[...])
        for i in range(2):
            row = logits[i * 256 : (i + 1) * 256]
            labels = labels_ref[2 * at + i].astype(single)
            spread = jnp.maximum(row, 0.0) + jnp.log1p(jnp.exp(-jnp.abs(row)))
            penalty = jnp.sum(spread - labels * row, axis=0, keepdims=True)
            loss_ref[2 * at + i] = jnp.broadcast_to(penalty, (8, 128))
            slope = ((jax.nn.sigmoid(row) - labels) * loss_weight).astype(bfloat)
            one = slice(i * 256, (i + 1) * 256)
            sum_head[...] += outer(out_fine[one], slope)
            level = logistic[one]
            down = backward(slope, head[...]) * (level * (1.0 + pre[one] * (1.0 - level)))
            put_row(field_fine, 2 * at + i + 1, down.astype(bfloat))

    fine_rows(top_step, True, False)
    take_edges(field_top, 16)
    fine_rows(top_step, False, True)
    g_head[...] = sum_head[...].astype(bfloat)
    fine_edges(field_fine, 1)
    send_edges(edges_fine.at[1, 0], edges_fine.at[1, 1], halo_fine, 5, 2)

    def fine_weight(field, grad_out):
        sum_fine[...] = jnp.zeros_like(sum_fine)

        def step(at):
            back = field_fine[window((2 * at + 1) * 256, 512), 128:256]
            sum_fine[...] += outer(back, tap_rows(field, 2 * at, 2, 256))

        each(0, 8, step)
        for k in range(9):
            part = sum_fine[:, k * 128 : (k + 1) * 128]
            grad_out[pl.ds(k * 128, 128), :] = part.T.astype(bfloat)

    fine_weight(field_top, g_top)
    take_edges(field_fine, 16)

    def grad_fine_step(at):
        value = times(tap_rows(field_fine, 2 * at, 2, 256), flip_top[...]).astype(bfloat)
        rows = window(at * 128, 128)
        for k in range(4):
            grad_fine[rows, k * 128 : (k + 1) * 128] = value[k * 128 : (k + 1) * 128]

    each(0, 8, grad_fine_step)

    def back_merge_step(at):
        rows = window(at * 256, 256)
        value = backward(grad_fine[rows, :], middle_up[...]) * silu_slope(pre_merge[rows, :])
        value = value.astype(bfloat)
        for k in range(2):
            put_row(field_middle, 2 * at + k + 1, value[k * 128 : (k + 1) * 128])

    each(0, 4, back_merge_step)
    middle_edges(field_middle, 2)
    send_edges(edges_middle.at[2, 0], edges_middle.at[2, 1], halo_middle, 6, 2)
    g_up[...] = outer(out_middle[...], grad_fine[...]).astype(bfloat)

    def middle_weight(field, grad_out):
        for part in range(3):
            total = jnp.zeros((256, 768), single)
            back = field_middle[pl.ds(128, 1024), 256:512]
            taps = field[pl.ds(part * 128, 1024), :]
            total = outer(back, taps)
            for k in range(3):
                grad_out[pl.ds(part * 768 + k * 256, 256), :] = (
                    total[:, k * 256 : (k + 1) * 256].T.astype(bfloat)
                )

    middle_weight(field_merge, g_merge)
    take_edges(field_middle, 8)

    def grad_middle_step(at):
        value = times(tap_rows(field_middle, 2 * at, 2, 128), flip_merge[...]).astype(bfloat)
        rows = window(at * 64, 64)
        for k in range(4):
            grad_middle[rows, k * 256 : (k + 1) * 256] = value[k * 64 : (k + 1) * 64]

    each(0, 4, grad_middle_step)

    value = backward(grad_middle[...], coarse_up[...]) * silu_slope(pre_coarse[...])
    spread_coarse(field_coarse, value.astype(bfloat), 1, 7)
    g_coarse_up[...] = outer(hid_coarse[...], grad_middle[...]).astype(bfloat)

    def coarse_weight(step):
        back = field_coarse[pl.ds(64, 256), 512:1024]
        total = outer(field_two[window(step * 64, 256), :], back)
        g_coarse[window(step * 1536, 1536), :] = total.astype(bfloat)

    each(0, 3, coarse_weight)
    take_edges(field_coarse, 4)
    pre_coarse[...] = coarse_part(field_coarse, flip_coarse, 1)

    def coarse_back(index):
        pre_coarse[...] += coarse_part(field_coarse, flip_coarse, 2 * index)

    each(0, 2, coarse_back)
    value = pre_coarse[...].astype(bfloat)

    hid_coarse[...] = value

    def back_middle_step(at):
        rows = window(at * 64, 64)
        total = backward(hid_coarse[rows, :], middle_down[...]) + grad_middle[rows, :].astype(single)
        total = (total * silu_slope(pre_middle[rows, :])).astype(bfloat)
        for i in range(2):
            row = jnp.concatenate(
                [total[:, (2 * i + j) * 256 : (2 * i + j + 1) * 256] for j in range(2)], axis=0
            )
            put_row(field_middle, 2 * at + i + 1, row)

    each(0, 4, back_middle_step)
    middle_edges(field_middle, 3)
    send_edges(edges_middle.at[3, 0], edges_middle.at[3, 1], halo_middle, 8, 3)
    g_middle_down[...] = outer(hid_middle[...], hid_coarse[...]).astype(bfloat)
    middle_weight(field_one, g_middle)
    take_edges(field_middle, 8)

    def grad_one_step(at):
        value = times(tap_rows(field_middle, 2 * at, 2, 128), flip_middle[...]).astype(bfloat)
        grad_one[window(at * 256, 256), :] = value

    each(0, 4, grad_one_step)

    def back_fine_step(at):
        rows = window(at * 128, 128)
        total = backward(grad_one[rows, :], fine_down[...]) + grad_fine[rows, :].astype(single)
        total = (total * silu_slope(pre_fine[rows, :])).astype(bfloat)
        for i in range(2):
            row = jnp.concatenate(
                [total[:, (2 * i + j) * 128 : (2 * i + j + 1) * 128] for j in range(2)], axis=0
            )
            put_row(field_fine, 2 * at + i + 1, row)

    each(0, 8, back_fine_step)
    fine_edges(field_fine, 2)
    send_edges(edges_fine.at[2, 0], edges_fine.at[2, 1], halo_fine, 9, 3)
    g_fine_down[...] = outer(hid_fine[...], grad_one[...]).astype(bfloat)
    fine_weight(field_zero, g_fine)
    take_edges(field_fine, 16)

    def zero_step(at):
        value = times(tap_rows(field_fine, 2 * at, 2, 256), flip_fine[...]).astype(bfloat)
        for i in range(2):
            zero_grad[2 * at + i] = value[i * 256 : (i + 1) * 256]

    each(0, 8, zero_step)

    for top, bottom, halo, exchange, slot in started:

        @pl.when(slab < last)
        def _():
            edge_copy(bottom, halo, exchange, slot, 0).wait_send()

        @pl.when(slab > 0)
        def _():
            edge_copy(top, halo, exchange, slot, 1).wait_send()


def unet(*operands):
    bfloat, single = jnp.bfloat16, jnp.float32
    shapes = [
        ((16, 256, 128), bfloat), ((16, 8, 128), single), ((1152, 128), bfloat),
        ((512, 256), bfloat), ((2304, 256), bfloat), ((1024, 512), bfloat),
        ((4608, 512), bfloat), ((512, 1024), bfloat), ((2304, 256), bfloat),
        ((256, 512), bfloat), ((1152, 128), bfloat), ((128, 128), bfloat),
    ]
    scratch = [
        ((18 * 256, 384), bfloat), ((18 * 256, 384), bfloat), ((18 * 256, 384), bfloat),
        ((10 * 128, 768), bfloat), ((10 * 128, 768), bfloat), ((10 * 128, 768), bfloat),
        ((6 * 64, 1536), bfloat), ((6 * 64, 1536), bfloat),
        ((1024, 512), single), ((1024, 512), bfloat),
        ((256, 1024), single), ((256, 1024), bfloat),
        ((256, 512), single), ((256, 512), bfloat),
        ((1024, 256), single), ((1024, 256), bfloat),
        ((1024, 512), bfloat), ((256, 1024), bfloat), ((1024, 256), bfloat),
        ((128, 1152), single), ((8, 128), single), ((128, 128), single),
        ((3, 2, 256, 128), bfloat), ((4, 2, 128, 256), bfloat), ((2, 2, 64, 512), bfloat),
        ((4, 2, 256, 128), bfloat), ((4, 2, 128, 256), bfloat), ((2, 2, 64, 512), bfloat),
    ]
    return pl.pallas_call(
        unet_kernel,
        out_shape=[jax.ShapeDtypeStruct(*leaf) for leaf in shapes],
        in_specs=[pl.BlockSpec(memory_space=pltpu.VMEM)] * len(operands),
        out_specs=[pl.BlockSpec(memory_space=pltpu.VMEM)] * len(shapes),
        scratch_shapes=[pltpu.VMEM(*leaf) for leaf in scratch]
        + [pltpu.SemaphoreType.DMA((10, 2)), pltpu.SemaphoreType.DMA((10, 2))],
        compiler_params=pltpu.CompilerParams(
            collective_id=0, has_side_effects=True, vmem_limit_bytes=67043328
        ),
        cost_estimate=pl.CostEstimate(
            flops=24_000_000_000, bytes_accessed=40_000_000, transcendentals=4_000_000
        ),
    )(*operands)


def scatter_jobs(shapes):
    order = [(4, 0, 96), (6, 0, None), (2, 0, None), (4, 96, 96), (3, 0, None), (5, 0, None)]
    order += [(4, 192, 96)] + [(at, 0, None) for at in (1, 7, 0, 8, 9)]
    return [(at, row, size or shapes[at][0], at == 4) for at, row, size in order]


def scatter_kernel(jobs, *refs):
    single = jnp.float32
    count = len(jobs)
    terms, refs = refs[:10], refs[10:]
    outs, refs = refs[:10], refs[10:]
    own, refs = refs[:count], refs[count:]
    landed, refs = refs[:count], refs[count:]
    partial, refs = refs[:count], refs[count:]
    final, refs = refs[:count], refs[count:]
    own_sem, send_one, receive_one, send_two, receive_two = refs
    slab = lax.axis_index("slab")
    y, z = slab // 4, slab % 4
    barrier = pltpu.get_barrier_semaphore()

    def peer(along_y, step):
        if along_y:
            spot = (y + step) % 4
            return spot, spot * 4 + z
        spot = (z + step) % 4
        return spot, y * 4 + spot

    for along_y in (True, False):
        for step in (1, 2, 3):
            pl.semaphore_signal(
                barrier,
                inc=1,
                device_id={"slab": peer(along_y, step)[1]},
                device_id_type=MESH,
            )
    pl.semaphore_wait(barrier, 6)

    def group(job, spot):
        at, row, size, along_y = jobs[job]
        rows = pl.ds(row, size)
        if along_y:
            return terms[at].at[spot, :, rows]
        return terms[at].at[:, spot, rows]

    def keep(job):
        return pltpu.make_async_copy(
            group(job, y if jobs[job][3] else z), own[job], own_sem.at[job]
        )

    def first(job, step):
        spot, target = peer(jobs[job][3], step)
        return pltpu.make_async_remote_copy(
            src_ref=group(job, spot),
            dst_ref=landed[job].at[step - 1],
            send_sem=send_one.at[job, step - 1],
            recv_sem=receive_one.at[job, step - 1],
            device_id={"slab": target},
            device_id_type=MESH,
        )

    def second(job, step):
        spot, target = peer(not jobs[job][3], step)
        return pltpu.make_async_remote_copy(
            src_ref=partial[job].at[spot],
            dst_ref=final[job].at[step - 1],
            send_sem=send_two.at[job, step - 1],
            recv_sem=receive_two.at[job, step - 1],
            device_id={"slab": target},
            device_id_type=MESH,
        )

    for job in range(count):
        for step in (2, 1, 3):
            first(job, step).start()
        keep(job).start()
    for job in range(count):
        keep(job).wait()
        for step in (1, 2, 3):
            first(job, step).wait_recv()

        def add(spot, carry, job=job):
            total = own[job][spot].astype(single)
            for step in range(3):
                total = total + landed[job][step, spot].astype(single)
            partial[job][spot] = total.astype(jnp.bfloat16)
            return carry

        lax.fori_loop(0, 4, add, 0)
        for step in (2, 1, 3):
            second(job, step).start()
    for job in range(count):
        at, row, size, along_y = jobs[job]
        for step in (1, 2, 3):
            second(job, step).wait_recv()
        total = partial[job][z if along_y else y].astype(single)
        for step in range(3):
            total = total + final[job][step].astype(single)
        outs[at][pl.ds(row, size), :] = total
    for job in range(count):
        for step in (1, 2, 3):
            first(job, step).wait_send()
            second(job, step).wait_send()


def scatter_sums(terms):
    bfloat = jnp.bfloat16
    shapes = [(term.shape[0] // 16, term.shape[1]) for term in terms]
    jobs = scatter_jobs(shapes)
    blocks = [(size, shapes[at][1]) for at, _, size, _ in jobs]
    scratch = [pltpu.VMEM((4, *block), bfloat) for block in blocks]
    scratch += [pltpu.VMEM((3, 4, *block), bfloat) for block in blocks]
    scratch += [pltpu.VMEM((4, *block), bfloat) for block in blocks]
    scratch += [pltpu.VMEM((3, *block), bfloat) for block in blocks]
    scratch += [pltpu.SemaphoreType.DMA((len(jobs),))]
    scratch += [pltpu.SemaphoreType.DMA((len(jobs), 3)) for _ in range(4)]
    return pl.pallas_call(
        functools.partial(scatter_kernel, jobs),
        out_shape=[jax.ShapeDtypeStruct(shape, jnp.float32) for shape in shapes],
        in_specs=[pl.BlockSpec(memory_space=pl.ANY)] * len(terms),
        out_specs=[pl.BlockSpec(memory_space=pltpu.VMEM)] * len(terms),
        scratch_shapes=scratch,
        compiler_params=pltpu.CompilerParams(
            collective_id=1, has_side_effects=True, vmem_limit_bytes=40000000
        ),
        cost_estimate=pl.CostEstimate(
            flops=2_000_000_000, bytes_accessed=30_000_000, transcendentals=0
        ),
    )(*[term.reshape(4, 4, *shape) for term, shape in zip(terms, shapes)])


def by_parity(field):
    rows, across, channels = field.shape
    return (
        field.reshape(rows, across // 4, 2, 2, channels)
        .transpose(0, 3, 2, 1, 4)
        .reshape(rows, across, channels)
    )


def body(
    camera_features,
    cell_index,
    owner_device,
    owner_tile,
    base_map,
    targets,
    fine_conv,
    fine_down,
    middle_conv,
    middle_down,
    coarse_conv,
    coarse_up,
    middle_merge,
    middle_up,
    fine_merge,
    head_weight,
):
    single = jnp.float32
    bfloat = jnp.bfloat16
    device = lax.axis_index("slab")
    devices = lax.axis_size("slab")
    height, across, channels = base_map.shape
    slot_count = devices * CAP
    tile_count = height * across // TILE
    owners = owner_device[:, 0]
    everyone = owners.shape[0]
    choose = (owners[:, None] == jnp.arange(devices, dtype=jnp.int32)[None, :]).astype(jnp.int32)
    grouped = choose.reshape(devices, BLK_DEV, devices)
    earlier = (jnp.cumsum(grouped, axis=1) - grouped).reshape(everyone, devices)
    ranking = jnp.sum(earlier * choose, axis=1)
    sources = jnp.arange(everyone, dtype=jnp.int32) // BLK_DEV
    slot_number = owners * CAP + ranking
    local_slot = lax.dynamic_slice_in_dim(slot_number, device * BLK_DEV, BLK_DEV)
    slot_range = jnp.arange(slot_count, dtype=jnp.int32)
    send_map = (local_slot[None, :] == slot_range[:, None]).astype(bfloat)
    arrival = sources * CAP + ranking
    receive_map = ((arrival[None, :] == slot_range[:, None]) & (owners[None, :] == device)).astype(
        jnp.int32
    )
    tile_onehot = (owner_tile[:, None] == jnp.arange(tile_count, dtype=jnp.int32)[None, :]).astype(
        jnp.int32
    )
    placement = jnp.einsum("bt,sb->ts", tile_onehot, receive_map).astype(bfloat)
    cell_range = jnp.arange(TILE, dtype=jnp.int32)
    local_cells = lax.dynamic_slice_in_dim(cell_index, device * BLK_DEV, BLK_DEV)
    local_cells = local_cells % 2 * 64 + local_cells // 2 % 2 * 32 + local_cells // 4
    cell_onehot = (local_cells[:, :, None] == cell_range[None, None, :]).astype(bfloat)
    payload = (
        jnp.einsum("bpt,bpc->btc", cell_onehot, camera_features, preferred_element_type=single)
        .astype(bfloat)
        .reshape(BLK_DEV, -1)
    )
    outgoing = (
        jnp.dot(send_map, payload, preferred_element_type=single)
        .astype(bfloat)
        .reshape(devices, CAP, -1)
    )
    incoming = lax.all_to_all(outgoing, "slab", split_axis=0, concat_axis=0, tiled=True).reshape(
        slot_count, -1
    )
    canvas = jnp.dot(placement, incoming, preferred_element_type=single)
    canvas = canvas.reshape(height, 2, 4, 32, channels).transpose(0, 2, 1, 3, 4)
    level_zero = (
        by_parity(base_map).astype(single) + canvas.reshape(height, across, channels)
    ).astype(bfloat)
    level_zero_grad, losses, *terms = unet(
        level_zero,
        by_parity(targets),
        fine_conv,
        fine_down,
        middle_conv,
        middle_down,
        coarse_conv,
        coarse_up,
        middle_merge,
        middle_up,
        fine_merge,
        head_weight,
        flipped(fine_conv),
        flipped(middle_conv),
        flipped(coarse_conv),
        flipped(middle_merge),
        flipped(fine_merge),
    )
    row_loss = jnp.sum(losses[:, 0, :], axis=1) / (across * K)
    level_zero_grad = level_zero_grad.reshape(height, 4, 2, 32, channels).transpose(0, 2, 1, 3, 4)
    tiles_grad = level_zero_grad.reshape(tile_count, -1)
    slot_grad = jnp.einsum(
        "ts,tl->sl", placement, tiles_grad, preferred_element_type=single
    ).astype(bfloat)
    returned = lax.all_to_all(
        slot_grad.reshape(devices, CAP, -1), "slab", split_axis=0, concat_axis=0, tiled=True
    ).reshape(slot_count, -1)
    own_blocks = jnp.einsum("sb,sl->bl", send_map, returned, preferred_element_type=single).astype(
        bfloat
    )
    camera_grad = jnp.einsum(
        "bpt,btc->bpc",
        cell_onehot,
        own_blocks.reshape(BLK_DEV, TILE, channels),
        preferred_element_type=single,
    ).astype(bfloat)
    sums = scatter_sums(terms)
    return (camera_grad, row_loss, *sums)


def solution(mesh):
    step = jax.shard_map(
        body,
        mesh=mesh,
        in_specs=(
            P(("scene", "slab"), None, None),
            P("scene", None),
            P("scene", None),
            P("scene"),
            P(("scene", "slab"), None, None),
            P(("scene", "slab"), None, None),
            P(),
            P(),
            P(),
            P(),
            P(),
            P(),
            P(),
            P(),
            P(),
            P(),
        ),
        out_specs=(
            P(("scene", "slab"), None, None),
            P(("scene", "slab")),
            P(("scene", "slab"), None),
            P(("scene", "slab"), None),
            P(("scene", "slab"), None),
            P(("scene", "slab"), None),
            P(("scene", "slab"), None),
            P(("scene", "slab"), None),
            P(("scene", "slab"), None),
            P(("scene", "slab"), None),
            P(("scene", "slab"), None),
            P(("scene", "slab"), None),
        ),
        check_vma=False,
    )
    return step
```

```python
import functools

import jax
import jax.numpy as jnp
from jax import lax
from jax.experimental import pallas as pl
from jax.experimental.pallas import tpu as pltpu
from jax.sharding import PartitionSpec as P

BLK_DEV = 64
C1 = 256
C2 = 512
K = 128
TILE = 128
CAP = 8
MESH = pl.DeviceIdType.MESH


loss_weight = 0.0625


def flipped(weight):
    inward = weight.shape[0] // 9
    return weight.reshape(9, inward, -1)[::-1].transpose(0, 2, 1).reshape(-1, inward)


def silu_slope(signal):
    logistic = jax.nn.sigmoid(signal)
    return logistic * (1.0 + signal * (1.0 - logistic))


def outer(former, latter):
    return lax.dot_general(
        former, latter, (((0,), (0,)), ((), ())), preferred_element_type=jnp.float32
    )


def backward(former, latter):
    return lax.dot_general(
        former, latter, (((1,), (1,)), ((), ())), preferred_element_type=jnp.float32
    )


def lower_rows(block):
    moved = pltpu.roll(block.astype(jnp.float32), 1, 0)
    place = lax.broadcasted_iota(jnp.int32, moved.shape, 0)
    return jnp.where(place == 0, 0.0, moved).astype(block.dtype)


def upper_rows(block):
    length = block.shape[0]
    moved = pltpu.roll(block.astype(jnp.float32), length - 1, 0)
    place = lax.broadcasted_iota(jnp.int32, moved.shape, 0)
    return jnp.where(place == length - 1, 0.0, moved).astype(block.dtype)


def shifted_pair(row):
    span = 64
    blocks = [row[at : at + span] for at in range(0, row.shape[0], span)]
    if len(blocks) == 1:
        return lower_rows(row), upper_rows(row)
    if len(blocks) == 2:
        left = [lower_rows(blocks[1]), blocks[0]]
        right = [blocks[1], upper_rows(blocks[0])]
    else:
        left = [lower_rows(blocks[3]), blocks[2], blocks[0], blocks[1]]
        right = [blocks[2], blocks[3], blocks[1], upper_rows(blocks[0])]
    return jnp.concatenate(left, axis=0), jnp.concatenate(right, axis=0)


def window(start, size):
    if isinstance(start, int):
        return pl.ds(start, size)
    return pl.ds(pl.multiple_of(start, size if size < 64 else 64), size)


def put_row(field, at, row):
    span, channels = row.shape
    left, right = shifted_pair(row)
    rows = window(at * span, span)
    field[rows, 0:channels] = left
    field[rows, channels : 2 * channels] = row
    field[rows, 2 * channels : 3 * channels] = right


def tap_rows(field, first, count, span):
    return jnp.concatenate(
        [field[window((first + step) * span, count * span), :] for step in range(3)], axis=1
    )


def times(former, latter):
    return jnp.dot(former, latter, preferred_element_type=jnp.float32)


def unet_kernel(*refs):
    (
        zero_ref, labels_ref, fine_conv, fine_down, middle_conv, middle_down, coarse_conv,
        coarse_up, middle_merge, middle_up, fine_merge, head, flip_fine, flip_middle,
        flip_coarse, flip_merge, flip_top,
        zero_grad, loss_ref, g_fine, g_fine_down, g_middle, g_middle_down, g_coarse,
        g_coarse_up, g_merge, g_up, g_top, g_head,
        field_zero, field_top, field_fine, field_one, field_merge, field_middle, field_two,
        field_coarse, pre_fine, hid_fine, pre_middle, hid_middle, pre_coarse, hid_coarse,
        pre_merge, out_middle, grad_fine, grad_middle, grad_one, sum_fine, sum_middle, sum_head,
        edges_fine, edges_middle, edges_coarse, halo_fine, halo_middle, halo_coarse,
        send_sem, receive_sem,
    ) = refs
    bfloat, single = jnp.bfloat16, jnp.float32
    slab = lax.axis_index("slab")
    last = lax.axis_size("slab") - 1
    barrier = pltpu.get_barrier_semaphore()

    for step in (1, last):
        pl.semaphore_signal(
            barrier,
            inc=1,
            device_id={"slab": lax.rem(slab + step, last + 1)},
            device_id_type=MESH,
        )
    pl.semaphore_wait(barrier, 2)

    def edge_copy(source, halo, exchange, slot, way):
        return pltpu.make_async_remote_copy(
            src_ref=source,
            dst_ref=halo.at[slot, way],
            send_sem=send_sem.at[exchange, way],
            recv_sem=receive_sem.at[exchange, way],
            device_id={"slab": slab + (1 if way == 0 else -1)},
            device_id_type=MESH,
        )

    started = []

    def send_edges(top, bottom, halo, exchange, slot):
        started.append((top, bottom, halo, exchange, slot))

        @pl.when(slab < last)
        def _():
            edge_copy(bottom, halo, exchange, slot, 0).start()

        @pl.when(slab > 0)
        def _():
            edge_copy(top, halo, exchange, slot, 1).start()

    def take_edges(field, height):
        top, bottom, halo, exchange, slot = started[-1]

        @pl.when(slab > 0)
        def _():
            edge_copy(bottom, halo, exchange, slot, 0).wait_recv()

        @pl.when(slab == 0)
        def _():
            halo[slot, 0] = jnp.zeros(halo.shape[2:], halo.dtype)

        @pl.when(slab < last)
        def _():
            edge_copy(top, halo, exchange, slot, 1).wait_recv()

        @pl.when(slab == last)
        def _():
            halo[slot, 1] = jnp.zeros(halo.shape[2:], halo.dtype)

        put_row(field, 0, halo[slot, 0])
        put_row(field, height + 1, halo[slot, 1])

    def each(first, bound, body):
        def step(index, carry):
            body(index)
            return carry

        lax.fori_loop(first, bound, step, 0)

    def fine_rows(handle, inner, outer_):
        if inner:
            each(1, 7, handle)
        if outer_:
            each(0, 2, lambda index: handle(index * 7))

    def middle_rows(handle, inner, outer_):
        if inner:
            each(1, 3, handle)
        if outer_:
            each(0, 2, lambda index: handle(index * 3))

    quads = [(0, 0), (0, 1), (1, 0), (1, 1)]

    send_edges(zero_ref.at[0], zero_ref.at[15], halo_fine, 0, 0)
    each(0, 16, lambda row: put_row(field_zero, row + 1, zero_ref[row]))

    def fine_step(at):
        pre = times(tap_rows(field_zero, 2 * at, 2, 256), fine_conv[...])
        rows = window(at * 128, 128)
        for k in range(4):
            part = pre[k * 128 : (k + 1) * 128]
            pre_fine[rows, k * 128 : (k + 1) * 128] = part
            hid_fine[rows, k * 128 : (k + 1) * 128] = jax.nn.silu(part).astype(bfloat)

    fine_rows(fine_step, True, False)
    take_edges(field_zero, 16)
    fine_rows(fine_step, False, True)

    def one_step(at):
        value = times(hid_fine[window(at * 256, 256), :], fine_down[...]).astype(bfloat)
        for k in range(2):
            put_row(field_one, 2 * at + k + 1, value[k * 128 : (k + 1) * 128])

    def middle_edges(field, slot):
        edges_middle[slot, 0] = field[pl.ds(128, 128), 256:512]
        edges_middle[slot, 1] = field[pl.ds(8 * 128, 128), 256:512]

    middle_rows(one_step, False, True)
    middle_edges(field_one, 0)
    send_edges(edges_middle.at[0, 0], edges_middle.at[0, 1], halo_middle, 1, 0)
    middle_rows(one_step, True, False)

    def middle_step(at):
        pre = times(tap_rows(field_one, 2 * at, 2, 128), middle_conv[...])
        rows = window(at * 64, 64)
        for k in range(4):
            part = pre[k * 64 : (k + 1) * 64]
            pre_middle[rows, k * 256 : (k + 1) * 256] = part
            hid_middle[rows, k * 256 : (k + 1) * 256] = jax.nn.silu(part).astype(bfloat)

    middle_rows(middle_step, True, False)
    take_edges(field_one, 8)
    middle_rows(middle_step, False, True)

    def spread_coarse(field, value, slot, exchange):
        for row in range(4):
            put_row(field, row + 1, value[row * 64 : (row + 1) * 64])
        edges_coarse[slot, 0] = value[0:64]
        edges_coarse[slot, 1] = value[192:256]
        send_edges(edges_coarse.at[slot, 0], edges_coarse.at[slot, 1], halo_coarse, exchange, slot)

    def coarse_part(field, weight, step):
        return times(
            field[window(step * 64, 256), :], weight[window(step * 1536, 1536), :]
        )

    value = times(hid_middle[...], middle_down[...]).astype(bfloat)
    spread_coarse(field_two, value, 0, 2)
    pre_coarse[...] = coarse_part(field_two, coarse_conv, 1)
    take_edges(field_two, 4)

    def coarse_step(index):
        pre_coarse[...] += coarse_part(field_two, coarse_conv, 2 * index)

    each(0, 2, coarse_step)
    hid_coarse[...] = jax.nn.silu(pre_coarse[...]).astype(bfloat)

    def join_middle(at):
        rows = window(at * 64, 64)
        total = times(hid_coarse[rows, :], coarse_up[...]) + hid_middle[rows, :].astype(single)
        total = total.astype(bfloat)
        for i in range(2):
            row = jnp.concatenate(
                [total[:, (2 * i + j) * 256 : (2 * i + j + 1) * 256] for j in range(2)], axis=0
            )
            put_row(field_merge, 2 * at + i + 1, row)

    middle_rows(join_middle, False, True)
    middle_edges(field_merge, 1)
    send_edges(edges_middle.at[1, 0], edges_middle.at[1, 1], halo_middle, 3, 1)
    middle_rows(join_middle, True, False)

    def merge_step(at):
        pre = times(tap_rows(field_merge, 2 * at, 2, 128), middle_merge[...])
        rows = window(at * 256, 256)
        pre_merge[rows, :] = pre
        out_middle[rows, :] = jax.nn.silu(pre).astype(bfloat)

    middle_rows(merge_step, True, False)
    take_edges(field_merge, 8)
    middle_rows(merge_step, False, True)

    def join_fine(at):
        rows = window(at * 128, 128)
        total = times(out_middle[rows, :], middle_up[...]) + hid_fine[rows, :].astype(single)
        total = total.astype(bfloat)
        for i in range(2):
            row = jnp.concatenate(
                [total[:, (2 * i + j) * 128 : (2 * i + j + 1) * 128] for j in range(2)], axis=0
            )
            put_row(field_top, 2 * at + i + 1, row)

    def fine_edges(field, slot):
        edges_fine[slot, 0] = field[pl.ds(256, 256), 128:256]
        edges_fine[slot, 1] = field[pl.ds(16 * 256, 256), 128:256]

    fine_rows(join_fine, False, True)
    fine_edges(field_top, 0)
    send_edges(edges_fine.at[0, 0], edges_fine.at[0, 1], halo_fine, 4, 1)
    fine_rows(join_fine, True, False)
    sum_head[...] = jnp.zeros_like(sum_head)

    def top_step(at):
        pre = times(tap_rows(field_top, 2 * at, 2, 256), fine_merge[...])
        logistic = jax.nn.sigmoid(pre)
        out_fine = (pre * logistic).astype(bfloat)
        logits = times(out_fine, head[...])
        for i in range(2):
            row = logits[i * 256 : (i + 1) * 256]
            labels = labels_ref[2 * at + i].astype(single)
            spread = jnp.maximum(row, 0.0) + jnp.log1p(jnp.exp(-jnp.abs(row)))
            penalty = jnp.sum(spread - labels * row, axis=0, keepdims=True)
            loss_ref[2 * at + i] = jnp.broadcast_to(penalty, (8, 128))
            slope = ((jax.nn.sigmoid(row) - labels) * loss_weight).astype(bfloat)
            one = slice(i * 256, (i + 1) * 256)
            sum_head[...] += outer(out_fine[one], slope)
            level = logistic[one]
            down = backward(slope, head[...]) * (level * (1.0 + pre[one] * (1.0 - level)))
            put_row(field_fine, 2 * at + i + 1, down.astype(bfloat))

    fine_rows(top_step, True, False)
    take_edges(field_top, 16)
    fine_rows(top_step, False, True)
    g_head[...] = sum_head[...].astype(bfloat)
    fine_edges(field_fine, 1)
    send_edges(edges_fine.at[1, 0], edges_fine.at[1, 1], halo_fine, 5, 2)

    def fine_weight(field, grad_out):
        sum_fine[...] = jnp.zeros_like(sum_fine)

        def step(at):
            back = field_fine[window((2 * at + 1) * 256, 512), 128:256]
            sum_fine[...] += outer(back, tap_rows(field, 2 * at, 2, 256))

        each(0, 8, step)
        for k in range(9):
            part = sum_fine[:, k * 128 : (k + 1) * 128]
            grad_out[pl.ds(k * 128, 128), :] = part.T.astype(bfloat)

    fine_weight(field_top, g_top)
    take_edges(field_fine, 16)

    def grad_fine_step(at):
        value = times(tap_rows(field_fine, 2 * at, 2, 256), flip_top[...]).astype(bfloat)
        rows = window(at * 128, 128)
        for k in range(4):
            grad_fine[rows, k * 128 : (k + 1) * 128] = value[k * 128 : (k + 1) * 128]

    each(0, 8, grad_fine_step)

    def back_merge_step(at):
        rows = window(at * 256, 256)
        value = backward(grad_fine[rows, :], middle_up[...]) * silu_slope(pre_merge[rows, :])
        value = value.astype(bfloat)
        for k in range(2):
            put_row(field_middle, 2 * at + k + 1, value[k * 128 : (k + 1) * 128])

    each(0, 4, back_merge_step)
    middle_edges(field_middle, 2)
    send_edges(edges_middle.at[2, 0], edges_middle.at[2, 1], halo_middle, 6, 2)
    g_up[...] = outer(out_middle[...], grad_fine[...]).astype(bfloat)

    def middle_weight(field, grad_out):
        for part in range(3):
            total = jnp.zeros((256, 768), single)
            back = field_middle[pl.ds(128, 1024), 256:512]
            taps = field[pl.ds(part * 128, 1024), :]
            total = outer(back, taps)
            for k in range(3):
                grad_out[pl.ds(part * 768 + k * 256, 256), :] = (
                    total[:, k * 256 : (k + 1) * 256].T.astype(bfloat)
                )

    middle_weight(field_merge, g_merge)
    take_edges(field_middle, 8)

    def grad_middle_step(at):
        value = times(tap_rows(field_middle, 2 * at, 2, 128), flip_merge[...]).astype(bfloat)
        rows = window(at * 64, 64)
        for k in range(4):
            grad_middle[rows, k * 256 : (k + 1) * 256] = value[k * 64 : (k + 1) * 64]

    each(0, 4, grad_middle_step)

    value = backward(grad_middle[...], coarse_up[...]) * silu_slope(pre_coarse[...])
    spread_coarse(field_coarse, value.astype(bfloat), 1, 7)
    g_coarse_up[...] = outer(hid_coarse[...], grad_middle[...]).astype(bfloat)

    def coarse_weight(step):
        back = field_coarse[pl.ds(64, 256), 512:1024]
        total = outer(field_two[window(step * 64, 256), :], back)
        g_coarse[window(step * 1536, 1536), :] = total.astype(bfloat)

    each(0, 3, coarse_weight)
    take_edges(field_coarse, 4)
    pre_coarse[...] = coarse_part(field_coarse, flip_coarse, 1)

    def coarse_back(index):
        pre_coarse[...] += coarse_part(field_coarse, flip_coarse, 2 * index)

    each(0, 2, coarse_back)
    value = pre_coarse[...].astype(bfloat)

    hid_coarse[...] = value

    def back_middle_step(at):
        rows = window(at * 64, 64)
        total = backward(hid_coarse[rows, :], middle_down[...]) + grad_middle[rows, :].astype(single)
        total = (total * silu_slope(pre_middle[rows, :])).astype(bfloat)
        for i in range(2):
            row = jnp.concatenate(
                [total[:, (2 * i + j) * 256 : (2 * i + j + 1) * 256] for j in range(2)], axis=0
            )
            put_row(field_middle, 2 * at + i + 1, row)

    each(0, 4, back_middle_step)
    middle_edges(field_middle, 3)
    send_edges(edges_middle.at[3, 0], edges_middle.at[3, 1], halo_middle, 8, 3)
    g_middle_down[...] = outer(hid_middle[...], hid_coarse[...]).astype(bfloat)
    middle_weight(field_one, g_middle)
    take_edges(field_middle, 8)

    def grad_one_step(at):
        value = times(tap_rows(field_middle, 2 * at, 2, 128), flip_middle[...]).astype(bfloat)
        grad_one[window(at * 256, 256), :] = value

    each(0, 4, grad_one_step)

    def back_fine_step(at):
        rows = window(at * 128, 128)
        total = backward(grad_one[rows, :], fine_down[...]) + grad_fine[rows, :].astype(single)
        total = (total * silu_slope(pre_fine[rows, :])).astype(bfloat)
        for i in range(2):
            row = jnp.concatenate(
                [total[:, (2 * i + j) * 128 : (2 * i + j + 1) * 128] for j in range(2)], axis=0
            )
            put_row(field_fine, 2 * at + i + 1, row)

    each(0, 8, back_fine_step)
    fine_edges(field_fine, 2)
    send_edges(edges_fine.at[2, 0], edges_fine.at[2, 1], halo_fine, 9, 3)
    g_fine_down[...] = outer(hid_fine[...], grad_one[...]).astype(bfloat)
    fine_weight(field_zero, g_fine)
    take_edges(field_fine, 16)

    def zero_step(at):
        value = times(tap_rows(field_fine, 2 * at, 2, 256), flip_fine[...]).astype(bfloat)
        for i in range(2):
            zero_grad[2 * at + i] = value[i * 256 : (i + 1) * 256]

    each(0, 8, zero_step)

    for top, bottom, halo, exchange, slot in started:

        @pl.when(slab < last)
        def _():
            edge_copy(bottom, halo, exchange, slot, 0).wait_send()

        @pl.when(slab > 0)
        def _():
            edge_copy(top, halo, exchange, slot, 1).wait_send()


def unet(*operands):
    bfloat, single = jnp.bfloat16, jnp.float32
    shapes = [
        ((16, 256, 128), bfloat), ((16, 8, 128), single), ((1152, 128), bfloat),
        ((512, 256), bfloat), ((2304, 256), bfloat), ((1024, 512), bfloat),
        ((4608, 512), bfloat), ((512, 1024), bfloat), ((2304, 256), bfloat),
        ((256, 512), bfloat), ((1152, 128), bfloat), ((128, 128), bfloat),
    ]
    scratch = [
        ((18 * 256, 384), bfloat), ((18 * 256, 384), bfloat), ((18 * 256, 384), bfloat),
        ((10 * 128, 768), bfloat), ((10 * 128, 768), bfloat), ((10 * 128, 768), bfloat),
        ((6 * 64, 1536), bfloat), ((6 * 64, 1536), bfloat),
        ((1024, 512), single), ((1024, 512), bfloat),
        ((256, 1024), single), ((256, 1024), bfloat),
        ((256, 512), single), ((256, 512), bfloat),
        ((1024, 256), single), ((1024, 256), bfloat),
        ((1024, 512), bfloat), ((256, 1024), bfloat), ((1024, 256), bfloat),
        ((128, 1152), single), ((8, 128), single), ((128, 128), single),
        ((3, 2, 256, 128), bfloat), ((4, 2, 128, 256), bfloat), ((2, 2, 64, 512), bfloat),
        ((4, 2, 256, 128), bfloat), ((4, 2, 128, 256), bfloat), ((2, 2, 64, 512), bfloat),
    ]
    return pl.pallas_call(
        unet_kernel,
        out_shape=[jax.ShapeDtypeStruct(*leaf) for leaf in shapes],
        in_specs=[pl.BlockSpec(memory_space=pltpu.VMEM)] * len(operands),
        out_specs=[pl.BlockSpec(memory_space=pltpu.VMEM)] * len(shapes),
        scratch_shapes=[pltpu.VMEM(*leaf) for leaf in scratch]
        + [pltpu.SemaphoreType.DMA((10, 2)), pltpu.SemaphoreType.DMA((10, 2))],
        compiler_params=pltpu.CompilerParams(
            collective_id=0, has_side_effects=True, vmem_limit_bytes=67043328
        ),
        cost_estimate=pl.CostEstimate(
            flops=24_000_000_000, bytes_accessed=40_000_000, transcendentals=4_000_000
        ),
    )(*operands)


def scatter_jobs(shapes):
    order = [(4, 0, 96), (6, 0, None), (2, 0, None), (4, 96, 96), (3, 0, None), (5, 0, None)]
    order += [(4, 192, 96)] + [(at, 0, None) for at in (1, 7, 0, 8, 9)]
    return [(at, row, size or shapes[at][0], at == 4) for at, row, size in order]


def scatter_kernel(jobs, *refs):
    single = jnp.float32
    count = len(jobs)
    terms, refs = refs[:10], refs[10:]
    outs, refs = refs[:10], refs[10:]
    own, refs = refs[:count], refs[count:]
    landed, refs = refs[:count], refs[count:]
    partial, refs = refs[:count], refs[count:]
    final, refs = refs[:count], refs[count:]
    own_sem, send_one, receive_one, send_two, receive_two = refs
    slab = lax.axis_index("slab")
    y, z = slab // 4, slab % 4
    barrier = pltpu.get_barrier_semaphore()

    def peer(along_y, step):
        if along_y:
            spot = (y + step) % 4
            return spot, spot * 4 + z
        spot = (z + step) % 4
        return spot, y * 4 + spot

    for along_y in (True, False):
        for step in (1, 2, 3):
            pl.semaphore_signal(
                barrier,
                inc=1,
                device_id={"slab": peer(along_y, step)[1]},
                device_id_type=MESH,
            )
    pl.semaphore_wait(barrier, 6)

    def group(job, spot):
        at, row, size, along_y = jobs[job]
        rows = pl.ds(row, size)
        if along_y:
            return terms[at].at[spot, :, rows]
        return terms[at].at[:, spot, rows]

    def keep(job):
        return pltpu.make_async_copy(
            group(job, y if jobs[job][3] else z), own[job], own_sem.at[job]
        )

    def first(job, step):
        spot, target = peer(jobs[job][3], step)
        return pltpu.make_async_remote_copy(
            src_ref=group(job, spot),
            dst_ref=landed[job].at[step - 1],
            send_sem=send_one.at[job, step - 1],
            recv_sem=receive_one.at[job, step - 1],
            device_id={"slab": target},
            device_id_type=MESH,
        )

    def second(job, step):
        spot, target = peer(not jobs[job][3], step)
        return pltpu.make_async_remote_copy(
            src_ref=partial[job].at[spot],
            dst_ref=final[job].at[step - 1],
            send_sem=send_two.at[job, step - 1],
            recv_sem=receive_two.at[job, step - 1],
            device_id={"slab": target},
            device_id_type=MESH,
        )

    for job in range(count):
        for step in (2, 1, 3):
            first(job, step).start()
        keep(job).start()
    for job in range(count):
        keep(job).wait()
        for step in (1, 2, 3):
            first(job, step).wait_recv()

        def add(spot, carry, job=job):
            total = own[job][spot].astype(single)
            for step in range(3):
                total = total + landed[job][step, spot].astype(single)
            partial[job][spot] = total.astype(jnp.bfloat16)
            return carry

        lax.fori_loop(0, 4, add, 0)
        for step in (2, 1, 3):
            second(job, step).start()
    for job in range(count):
        at, row, size, along_y = jobs[job]
        for step in (1, 2, 3):
            second(job, step).wait_recv()
        total = partial[job][z if along_y else y].astype(single)
        for step in range(3):
            total = total + final[job][step].astype(single)
        outs[at][pl.ds(row, size), :] = total
    for job in range(count):
        for step in (1, 2, 3):
            first(job, step).wait_send()
            second(job, step).wait_send()


def hand_over(*refs):
    count = len(refs) // 2
    semaphores = refs[-1]
    copies = [
        pltpu.make_async_copy(refs[k], refs[count + k], semaphores.at[k]) for k in range(count)
    ]
    for copy in copies:
        copy.start()
    for copy in copies:
        copy.wait()


def scatter_sums(terms):
    bfloat = jnp.bfloat16
    shapes = [(term.shape[0] // 16, term.shape[1]) for term in terms]
    jobs = scatter_jobs(shapes)
    blocks = [(size, shapes[at][1]) for at, _, size, _ in jobs]
    scratch = [pltpu.VMEM((4, *block), bfloat) for block in blocks]
    scratch += [pltpu.VMEM((3, 4, *block), bfloat) for block in blocks]
    scratch += [pltpu.VMEM((4, *block), bfloat) for block in blocks]
    scratch += [pltpu.VMEM((3, *block), bfloat) for block in blocks]
    scratch += [pltpu.SemaphoreType.DMA((len(jobs),))]
    scratch += [pltpu.SemaphoreType.DMA((len(jobs), 3)) for _ in range(4)]
    sums = pl.pallas_call(
        functools.partial(scatter_kernel, jobs),
        out_shape=[jax.ShapeDtypeStruct(shape, jnp.float32) for shape in shapes],
        in_specs=[pl.BlockSpec(memory_space=pl.ANY)] * len(terms),
        out_specs=[pl.BlockSpec(memory_space=pltpu.VMEM)] * len(terms),
        scratch_shapes=scratch,
        compiler_params=pltpu.CompilerParams(
            collective_id=1, has_side_effects=True, vmem_limit_bytes=67043328
        ),
        cost_estimate=pl.CostEstimate(
            flops=2_000_000_000, bytes_accessed=30_000_000, transcendentals=0
        ),
    )(*[term.reshape(4, 4, *shape) for term, shape in zip(terms, shapes)])
    return pl.pallas_call(
        hand_over,
        out_shape=[jax.ShapeDtypeStruct(shape, jnp.float32) for shape in shapes],
        in_specs=[pl.BlockSpec(memory_space=pltpu.VMEM)] * len(sums),
        out_specs=[pl.BlockSpec(memory_space=pl.ANY)] * len(sums),
        scratch_shapes=[pltpu.SemaphoreType.DMA((len(sums),))],
        compiler_params=pltpu.CompilerParams(vmem_limit_bytes=67043328),
    )(*sums)


def by_parity(field):
    rows, across, channels = field.shape
    return (
        field.reshape(rows, across // 4, 2, 2, channels)
        .transpose(0, 3, 2, 1, 4)
        .reshape(rows, across, channels)
    )


def body(
    camera_features,
    cell_index,
    owner_device,
    owner_tile,
    base_map,
    targets,
    fine_conv,
    fine_down,
    middle_conv,
    middle_down,
    coarse_conv,
    coarse_up,
    middle_merge,
    middle_up,
    fine_merge,
    head_weight,
):
    single = jnp.float32
    bfloat = jnp.bfloat16
    device = lax.axis_index("slab")
    devices = lax.axis_size("slab")
    height, across, channels = base_map.shape
    slot_count = devices * CAP
    tile_count = height * across // TILE
    owners = owner_device[:, 0]
    everyone = owners.shape[0]
    choose = (owners[:, None] == jnp.arange(devices, dtype=jnp.int32)[None, :]).astype(jnp.int32)
    grouped = choose.reshape(devices, BLK_DEV, devices)
    earlier = (jnp.cumsum(grouped, axis=1) - grouped).reshape(everyone, devices)
    ranking = jnp.sum(earlier * choose, axis=1)
    sources = jnp.arange(everyone, dtype=jnp.int32) // BLK_DEV
    slot_number = owners * CAP + ranking
    local_slot = lax.dynamic_slice_in_dim(slot_number, device * BLK_DEV, BLK_DEV)
    slot_range = jnp.arange(slot_count, dtype=jnp.int32)
    send_map = (local_slot[None, :] == slot_range[:, None]).astype(bfloat)
    arrival = sources * CAP + ranking
    receive_map = ((arrival[None, :] == slot_range[:, None]) & (owners[None, :] == device)).astype(
        jnp.int32
    )
    tile_onehot = (owner_tile[:, None] == jnp.arange(tile_count, dtype=jnp.int32)[None, :]).astype(
        jnp.int32
    )
    placement = jnp.einsum("bt,sb->ts", tile_onehot, receive_map).astype(bfloat)
    cell_range = jnp.arange(TILE, dtype=jnp.int32)
    local_cells = lax.dynamic_slice_in_dim(cell_index, device * BLK_DEV, BLK_DEV)
    local_cells = local_cells % 2 * 64 + local_cells // 2 % 2 * 32 + local_cells // 4
    cell_onehot = (local_cells[:, :, None] == cell_range[None, None, :]).astype(bfloat)
    payload = (
        jnp.einsum("bpt,bpc->btc", cell_onehot, camera_features, preferred_element_type=single)
        .astype(bfloat)
        .reshape(BLK_DEV, -1)
    )
    outgoing = (
        jnp.dot(send_map, payload, preferred_element_type=single)
        .astype(bfloat)
        .reshape(devices, CAP, -1)
    )
    incoming = lax.all_to_all(outgoing, "slab", split_axis=0, concat_axis=0, tiled=True).reshape(
        slot_count, -1
    )
    canvas = jnp.dot(placement, incoming, preferred_element_type=single)
    canvas = canvas.reshape(height, 2, 4, 32, channels).transpose(0, 2, 1, 3, 4)
    level_zero = (
        by_parity(base_map).astype(single) + canvas.reshape(height, across, channels)
    ).astype(bfloat)
    level_zero_grad, losses, *terms = unet(
        level_zero,
        by_parity(targets),
        fine_conv,
        fine_down,
        middle_conv,
        middle_down,
        coarse_conv,
        coarse_up,
        middle_merge,
        middle_up,
        fine_merge,
        head_weight,
        flipped(fine_conv),
        flipped(middle_conv),
        flipped(coarse_conv),
        flipped(middle_merge),
        flipped(fine_merge),
    )
    row_loss = jnp.sum(losses[:, 0, :], axis=1) / (across * K)
    level_zero_grad = level_zero_grad.reshape(height, 4, 2, 32, channels).transpose(0, 2, 1, 3, 4)
    tiles_grad = level_zero_grad.reshape(tile_count, -1)
    slot_grad = jnp.einsum(
        "ts,tl->sl", placement, tiles_grad, preferred_element_type=single
    ).astype(bfloat)
    returned = lax.all_to_all(
        slot_grad.reshape(devices, CAP, -1), "slab", split_axis=0, concat_axis=0, tiled=True
    ).reshape(slot_count, -1)
    own_blocks = jnp.einsum("sb,sl->bl", send_map, returned, preferred_element_type=single).astype(
        bfloat
    )
    camera_grad = jnp.einsum(
        "bpt,btc->bpc",
        cell_onehot,
        own_blocks.reshape(BLK_DEV, TILE, channels),
        preferred_element_type=single,
    ).astype(bfloat)
    sums = scatter_sums(terms)
    return (camera_grad, row_loss, *sums)


def solution(mesh):
    step = jax.shard_map(
        body,
        mesh=mesh,
        in_specs=(
            P(("scene", "slab"), None, None),
            P("scene", None),
            P("scene", None),
            P("scene"),
            P(("scene", "slab"), None, None),
            P(("scene", "slab"), None, None),
            P(),
            P(),
            P(),
            P(),
            P(),
            P(),
            P(),
            P(),
            P(),
            P(),
        ),
        out_specs=(
            P(("scene", "slab"), None, None),
            P(("scene", "slab")),
            P(("scene", "slab"), None),
            P(("scene", "slab"), None),
            P(("scene", "slab"), None),
            P(("scene", "slab"), None),
            P(("scene", "slab"), None),
            P(("scene", "slab"), None),
            P(("scene", "slab"), None),
            P(("scene", "slab"), None),
            P(("scene", "slab"), None),
            P(("scene", "slab"), None),
        ),
        check_vma=False,
    )
    return step
```

```python
import functools

import jax
import jax.numpy as jnp
from jax import lax
from jax.experimental import pallas as pl
from jax.experimental.pallas import tpu as pltpu
from jax.sharding import PartitionSpec as P

BLK_DEV = 64
C1 = 256
C2 = 512
K = 128
TILE = 128
CAP = 8
MESH = pl.DeviceIdType.MESH


loss_weight = 0.0625


def flipped(weight):
    inward = weight.shape[0] // 9
    return weight.reshape(9, inward, -1)[::-1].transpose(0, 2, 1).reshape(-1, inward)


def silu_slope(signal):
    logistic = jax.nn.sigmoid(signal)
    return logistic * (1.0 + signal * (1.0 - logistic))


def outer(former, latter):
    return lax.dot_general(
        former, latter, (((0,), (0,)), ((), ())), preferred_element_type=jnp.float32
    )


def backward(former, latter):
    return lax.dot_general(
        former, latter, (((1,), (1,)), ((), ())), preferred_element_type=jnp.float32
    )


def lower_rows(block):
    moved = pltpu.roll(block.astype(jnp.float32), 1, 0)
    place = lax.broadcasted_iota(jnp.int32, moved.shape, 0)
    return jnp.where(place == 0, 0.0, moved).astype(block.dtype)


def upper_rows(block):
    length = block.shape[0]
    moved = pltpu.roll(block.astype(jnp.float32), length - 1, 0)
    place = lax.broadcasted_iota(jnp.int32, moved.shape, 0)
    return jnp.where(place == length - 1, 0.0, moved).astype(block.dtype)


def shifted_pair(row):
    span = 64
    blocks = [row[at : at + span] for at in range(0, row.shape[0], span)]
    if len(blocks) == 1:
        return lower_rows(row), upper_rows(row)
    if len(blocks) == 2:
        left = [lower_rows(blocks[1]), blocks[0]]
        right = [blocks[1], upper_rows(blocks[0])]
    else:
        left = [lower_rows(blocks[3]), blocks[2], blocks[0], blocks[1]]
        right = [blocks[2], blocks[3], blocks[1], upper_rows(blocks[0])]
    return jnp.concatenate(left, axis=0), jnp.concatenate(right, axis=0)


def window(start, size):
    if isinstance(start, int):
        return pl.ds(start, size)
    return pl.ds(pl.multiple_of(start, size if size < 64 else 64), size)


def put_row(field, at, row):
    span, channels = row.shape
    left, right = shifted_pair(row)
    rows = window(at * span, span)
    field[rows, 0:channels] = left
    field[rows, channels : 2 * channels] = row
    field[rows, 2 * channels : 3 * channels] = right


def tap_rows(field, first, count, span):
    return jnp.concatenate(
        [field[window((first + step) * span, count * span), :] for step in range(3)], axis=1
    )


def times(former, latter):
    return jnp.dot(former, latter, preferred_element_type=jnp.float32)


def unet_kernel(*refs):
    (
        zero_ref, labels_ref, fine_conv, fine_down, middle_conv, middle_down, coarse_conv,
        coarse_up, middle_merge, middle_up, fine_merge, head, flip_fine, flip_middle,
        flip_coarse, flip_merge, flip_top,
        zero_grad, loss_ref, g_fine, g_fine_down, g_middle, g_middle_down, g_coarse,
        g_coarse_up, g_merge, g_up, g_top, g_head,
        field_zero, field_top, field_fine, field_one, field_merge, field_middle, field_two,
        field_coarse, pre_fine, hid_fine, pre_middle, hid_middle, pre_coarse, hid_coarse,
        pre_merge, out_middle, grad_fine, grad_middle, grad_one, sum_fine, sum_middle, sum_head,
        edges_fine, edges_middle, edges_coarse, halo_fine, halo_middle, halo_coarse,
        send_sem, receive_sem,
    ) = refs
    bfloat, single = jnp.bfloat16, jnp.float32
    slab = lax.axis_index("slab")
    last = lax.axis_size("slab") - 1
    barrier = pltpu.get_barrier_semaphore()

    for step in (1, last):
        pl.semaphore_signal(
            barrier,
            inc=1,
            device_id={"slab": lax.rem(slab + step, last + 1)},
            device_id_type=MESH,
        )
    pl.semaphore_wait(barrier, 2)

    def edge_copy(source, halo, exchange, slot, way):
        return pltpu.make_async_remote_copy(
            src_ref=source,
            dst_ref=halo.at[slot, way],
            send_sem=send_sem.at[exchange, way],
            recv_sem=receive_sem.at[exchange, way],
            device_id={"slab": slab + (1 if way == 0 else -1)},
            device_id_type=MESH,
        )

    started = []

    def send_edges(top, bottom, halo, exchange, slot):
        started.append((top, bottom, halo, exchange, slot))

        @pl.when(slab < last)
        def _():
            edge_copy(bottom, halo, exchange, slot, 0).start()

        @pl.when(slab > 0)
        def _():
            edge_copy(top, halo, exchange, slot, 1).start()

    def take_edges(field, height):
        top, bottom, halo, exchange, slot = started[-1]

        @pl.when(slab > 0)
        def _():
            edge_copy(bottom, halo, exchange, slot, 0).wait_recv()

        @pl.when(slab == 0)
        def _():
            halo[slot, 0] = jnp.zeros(halo.shape[2:], halo.dtype)

        @pl.when(slab < last)
        def _():
            edge_copy(top, halo, exchange, slot, 1).wait_recv()

        @pl.when(slab == last)
        def _():
            halo[slot, 1] = jnp.zeros(halo.shape[2:], halo.dtype)

        put_row(field, 0, halo[slot, 0])
        put_row(field, height + 1, halo[slot, 1])

    def each(first, bound, body):
        def step(index, carry):
            body(index)
            return carry

        lax.fori_loop(first, bound, step, 0)

    def fine_rows(handle, inner, outer_):
        if inner:
            each(1, 7, handle)
        if outer_:
            each(0, 2, lambda index: handle(index * 7))

    def middle_rows(handle, inner, outer_):
        if inner:
            each(1, 3, handle)
        if outer_:
            each(0, 2, lambda index: handle(index * 3))

    quads = [(0, 0), (0, 1), (1, 0), (1, 1)]

    send_edges(zero_ref.at[0], zero_ref.at[15], halo_fine, 0, 0)
    each(0, 16, lambda row: put_row(field_zero, row + 1, zero_ref[row]))

    def fine_step(at):
        pre = times(tap_rows(field_zero, 2 * at, 2, 256), fine_conv[...])
        rows = window(at * 128, 128)
        for k in range(4):
            part = pre[k * 128 : (k + 1) * 128]
            pre_fine[rows, k * 128 : (k + 1) * 128] = part
            hid_fine[rows, k * 128 : (k + 1) * 128] = jax.nn.silu(part).astype(bfloat)

    fine_rows(fine_step, True, False)
    take_edges(field_zero, 16)
    fine_rows(fine_step, False, True)

    def one_step(at):
        value = times(hid_fine[window(at * 256, 256), :], fine_down[...]).astype(bfloat)
        for k in range(2):
            put_row(field_one, 2 * at + k + 1, value[k * 128 : (k + 1) * 128])

    def middle_edges(field, slot):
        edges_middle[slot, 0] = field[pl.ds(128, 128), 256:512]
        edges_middle[slot, 1] = field[pl.ds(8 * 128, 128), 256:512]

    middle_rows(one_step, False, True)
    middle_edges(field_one, 0)
    send_edges(edges_middle.at[0, 0], edges_middle.at[0, 1], halo_middle, 1, 0)
    middle_rows(one_step, True, False)

    def middle_step(at):
        pre = times(tap_rows(field_one, 2 * at, 2, 128), middle_conv[...])
        rows = window(at * 64, 64)
        for k in range(4):
            part = pre[k * 64 : (k + 1) * 64]
            pre_middle[rows, k * 256 : (k + 1) * 256] = part
            hid_middle[rows, k * 256 : (k + 1) * 256] = jax.nn.silu(part).astype(bfloat)

    middle_rows(middle_step, True, False)
    take_edges(field_one, 8)
    middle_rows(middle_step, False, True)

    def spread_coarse(field, value, slot, exchange):
        for row in range(4):
            put_row(field, row + 1, value[row * 64 : (row + 1) * 64])
        edges_coarse[slot, 0] = value[0:64]
        edges_coarse[slot, 1] = value[192:256]
        send_edges(edges_coarse.at[slot, 0], edges_coarse.at[slot, 1], halo_coarse, exchange, slot)

    def coarse_part(field, weight, step):
        return times(
            field[window(step * 64, 256), :], weight[window(step * 1536, 1536), :]
        )

    value = times(hid_middle[...], middle_down[...]).astype(bfloat)
    spread_coarse(field_two, value, 0, 2)
    pre_coarse[...] = coarse_part(field_two, coarse_conv, 1)
    take_edges(field_two, 4)

    def coarse_step(index):
        pre_coarse[...] += coarse_part(field_two, coarse_conv, 2 * index)

    each(0, 2, coarse_step)
    hid_coarse[...] = jax.nn.silu(pre_coarse[...]).astype(bfloat)

    def join_middle(at):
        rows = window(at * 64, 64)
        total = times(hid_coarse[rows, :], coarse_up[...]) + hid_middle[rows, :].astype(single)
        total = total.astype(bfloat)
        for i in range(2):
            row = jnp.concatenate(
                [total[:, (2 * i + j) * 256 : (2 * i + j + 1) * 256] for j in range(2)], axis=0
            )
            put_row(field_merge, 2 * at + i + 1, row)

    middle_rows(join_middle, False, True)
    middle_edges(field_merge, 1)
    send_edges(edges_middle.at[1, 0], edges_middle.at[1, 1], halo_middle, 3, 1)
    middle_rows(join_middle, True, False)

    def merge_step(at):
        pre = times(tap_rows(field_merge, 2 * at, 2, 128), middle_merge[...])
        rows = window(at * 256, 256)
        pre_merge[rows, :] = pre
        out_middle[rows, :] = jax.nn.silu(pre).astype(bfloat)

    middle_rows(merge_step, True, False)
    take_edges(field_merge, 8)
    middle_rows(merge_step, False, True)

    def join_fine(at):
        rows = window(at * 128, 128)
        total = times(out_middle[rows, :], middle_up[...]) + hid_fine[rows, :].astype(single)
        total = total.astype(bfloat)
        for i in range(2):
            row = jnp.concatenate(
                [total[:, (2 * i + j) * 128 : (2 * i + j + 1) * 128] for j in range(2)], axis=0
            )
            put_row(field_top, 2 * at + i + 1, row)

    def fine_edges(field, slot):
        edges_fine[slot, 0] = field[pl.ds(256, 256), 128:256]
        edges_fine[slot, 1] = field[pl.ds(16 * 256, 256), 128:256]

    fine_rows(join_fine, False, True)
    fine_edges(field_top, 0)
    send_edges(edges_fine.at[0, 0], edges_fine.at[0, 1], halo_fine, 4, 1)
    fine_rows(join_fine, True, False)
    sum_head[...] = jnp.zeros_like(sum_head)

    def top_step(at):
        pre = times(tap_rows(field_top, 2 * at, 2, 256), fine_merge[...])
        logistic = jax.nn.sigmoid(pre)
        out_fine = (pre * logistic).astype(bfloat)
        logits = times(out_fine, head[...])
        for i in range(2):
            row = logits[i * 256 : (i + 1) * 256]
            labels = labels_ref[2 * at + i].astype(single)
            spread = jnp.maximum(row, 0.0) + jnp.log1p(jnp.exp(-jnp.abs(row)))
            penalty = jnp.sum(spread - labels * row, axis=0, keepdims=True)
            loss_ref[2 * at + i] = jnp.broadcast_to(penalty, (8, 128))
            slope = ((jax.nn.sigmoid(row) - labels) * loss_weight).astype(bfloat)
            one = slice(i * 256, (i + 1) * 256)
            sum_head[...] += outer(out_fine[one], slope)
            level = logistic[one]
            down = backward(slope, head[...]) * (level * (1.0 + pre[one] * (1.0 - level)))
            put_row(field_fine, 2 * at + i + 1, down.astype(bfloat))

    fine_rows(top_step, True, False)
    take_edges(field_top, 16)
    fine_rows(top_step, False, True)
    g_head[...] = sum_head[...].astype(bfloat)
    fine_edges(field_fine, 1)
    send_edges(edges_fine.at[1, 0], edges_fine.at[1, 1], halo_fine, 5, 2)

    def fine_weight(field, grad_out):
        sum_fine[...] = jnp.zeros_like(sum_fine)

        def step(at):
            back = field_fine[window((2 * at + 1) * 256, 512), 128:256]
            sum_fine[...] += outer(back, tap_rows(field, 2 * at, 2, 256))

        each(0, 8, step)
        for k in range(9):
            part = sum_fine[:, k * 128 : (k + 1) * 128]
            grad_out[pl.ds(k * 128, 128), :] = part.T.astype(bfloat)

    fine_weight(field_top, g_top)
    take_edges(field_fine, 16)

    def grad_fine_step(at):
        value = times(tap_rows(field_fine, 2 * at, 2, 256), flip_top[...]).astype(bfloat)
        rows = window(at * 128, 128)
        for k in range(4):
            grad_fine[rows, k * 128 : (k + 1) * 128] = value[k * 128 : (k + 1) * 128]

    each(0, 8, grad_fine_step)

    def back_merge_step(at):
        rows = window(at * 256, 256)
        value = backward(grad_fine[rows, :], middle_up[...]) * silu_slope(pre_merge[rows, :])
        value = value.astype(bfloat)
        for k in range(2):
            put_row(field_middle, 2 * at + k + 1, value[k * 128 : (k + 1) * 128])

    each(0, 4, back_merge_step)
    middle_edges(field_middle, 2)
    send_edges(edges_middle.at[2, 0], edges_middle.at[2, 1], halo_middle, 6, 2)
    g_up[...] = outer(out_middle[...], grad_fine[...]).astype(bfloat)

    def middle_weight(field, grad_out):
        for part in range(3):
            total = jnp.zeros((256, 768), single)
            back = field_middle[pl.ds(128, 1024), 256:512]
            taps = field[pl.ds(part * 128, 1024), :]
            total = outer(back, taps)
            for k in range(3):
                grad_out[pl.ds(part * 768 + k * 256, 256), :] = (
                    total[:, k * 256 : (k + 1) * 256].T.astype(bfloat)
                )

    middle_weight(field_merge, g_merge)
    take_edges(field_middle, 8)

    def grad_middle_step(at):
        value = times(tap_rows(field_middle, 2 * at, 2, 128), flip_merge[...]).astype(bfloat)
        rows = window(at * 64, 64)
        for k in range(4):
            grad_middle[rows, k * 256 : (k + 1) * 256] = value[k * 64 : (k + 1) * 64]

    each(0, 4, grad_middle_step)

    value = backward(grad_middle[...], coarse_up[...]) * silu_slope(pre_coarse[...])
    spread_coarse(field_coarse, value.astype(bfloat), 1, 7)
    g_coarse_up[...] = outer(hid_coarse[...], grad_middle[...]).astype(bfloat)

    def coarse_weight(step):
        back = field_coarse[pl.ds(64, 256), 512:1024]
        total = outer(field_two[window(step * 64, 256), :], back)
        g_coarse[window(step * 1536, 1536), :] = total.astype(bfloat)

    each(0, 3, coarse_weight)
    take_edges(field_coarse, 4)
    pre_coarse[...] = coarse_part(field_coarse, flip_coarse, 1)

    def coarse_back(index):
        pre_coarse[...] += coarse_part(field_coarse, flip_coarse, 2 * index)

    each(0, 2, coarse_back)
    value = pre_coarse[...].astype(bfloat)

    hid_coarse[...] = value

    def back_middle_step(at):
        rows = window(at * 64, 64)
        total = backward(hid_coarse[rows, :], middle_down[...]) + grad_middle[rows, :].astype(single)
        total = (total * silu_slope(pre_middle[rows, :])).astype(bfloat)
        for i in range(2):
            row = jnp.concatenate(
                [total[:, (2 * i + j) * 256 : (2 * i + j + 1) * 256] for j in range(2)], axis=0
            )
            put_row(field_middle, 2 * at + i + 1, row)

    each(0, 4, back_middle_step)
    middle_edges(field_middle, 3)
    send_edges(edges_middle.at[3, 0], edges_middle.at[3, 1], halo_middle, 8, 3)
    g_middle_down[...] = outer(hid_middle[...], hid_coarse[...]).astype(bfloat)
    middle_weight(field_one, g_middle)
    take_edges(field_middle, 8)

    def grad_one_step(at):
        value = times(tap_rows(field_middle, 2 * at, 2, 128), flip_middle[...]).astype(bfloat)
        grad_one[window(at * 256, 256), :] = value

    each(0, 4, grad_one_step)

    def back_fine_step(at):
        rows = window(at * 128, 128)
        total = backward(grad_one[rows, :], fine_down[...]) + grad_fine[rows, :].astype(single)
        total = (total * silu_slope(pre_fine[rows, :])).astype(bfloat)
        for i in range(2):
            row = jnp.concatenate(
                [total[:, (2 * i + j) * 128 : (2 * i + j + 1) * 128] for j in range(2)], axis=0
            )
            put_row(field_fine, 2 * at + i + 1, row)

    each(0, 8, back_fine_step)
    fine_edges(field_fine, 2)
    send_edges(edges_fine.at[2, 0], edges_fine.at[2, 1], halo_fine, 9, 3)
    g_fine_down[...] = outer(hid_fine[...], grad_one[...]).astype(bfloat)
    fine_weight(field_zero, g_fine)
    take_edges(field_fine, 16)

    def zero_step(at):
        value = times(tap_rows(field_fine, 2 * at, 2, 256), flip_fine[...]).astype(bfloat)
        for i in range(2):
            zero_grad[2 * at + i] = value[i * 256 : (i + 1) * 256]

    each(0, 8, zero_step)

    for top, bottom, halo, exchange, slot in started:

        @pl.when(slab < last)
        def _():
            edge_copy(bottom, halo, exchange, slot, 0).wait_send()

        @pl.when(slab > 0)
        def _():
            edge_copy(top, halo, exchange, slot, 1).wait_send()


def unet(*operands):
    bfloat, single = jnp.bfloat16, jnp.float32
    shapes = [
        ((16, 256, 128), bfloat), ((16, 8, 128), single), ((1152, 128), bfloat),
        ((512, 256), bfloat), ((2304, 256), bfloat), ((1024, 512), bfloat),
        ((4608, 512), bfloat), ((512, 1024), bfloat), ((2304, 256), bfloat),
        ((256, 512), bfloat), ((1152, 128), bfloat), ((128, 128), bfloat),
    ]
    scratch = [
        ((18 * 256, 384), bfloat), ((18 * 256, 384), bfloat), ((18 * 256, 384), bfloat),
        ((10 * 128, 768), bfloat), ((10 * 128, 768), bfloat), ((10 * 128, 768), bfloat),
        ((6 * 64, 1536), bfloat), ((6 * 64, 1536), bfloat),
        ((1024, 512), single), ((1024, 512), bfloat),
        ((256, 1024), single), ((256, 1024), bfloat),
        ((256, 512), single), ((256, 512), bfloat),
        ((1024, 256), single), ((1024, 256), bfloat),
        ((1024, 512), bfloat), ((256, 1024), bfloat), ((1024, 256), bfloat),
        ((128, 1152), single), ((8, 128), single), ((128, 128), single),
        ((3, 2, 256, 128), bfloat), ((4, 2, 128, 256), bfloat), ((2, 2, 64, 512), bfloat),
        ((4, 2, 256, 128), bfloat), ((4, 2, 128, 256), bfloat), ((2, 2, 64, 512), bfloat),
    ]
    return pl.pallas_call(
        unet_kernel,
        out_shape=[jax.ShapeDtypeStruct(*leaf) for leaf in shapes],
        in_specs=[pl.BlockSpec(memory_space=pltpu.VMEM)] * len(operands),
        out_specs=[pl.BlockSpec(memory_space=pltpu.VMEM)] * len(shapes),
        scratch_shapes=[pltpu.VMEM(*leaf) for leaf in scratch]
        + [pltpu.SemaphoreType.DMA((10, 2)), pltpu.SemaphoreType.DMA((10, 2))],
        compiler_params=pltpu.CompilerParams(
            collective_id=0, has_side_effects=True, vmem_limit_bytes=67043328
        ),
        cost_estimate=pl.CostEstimate(
            flops=24_000_000_000, bytes_accessed=40_000_000, transcendentals=4_000_000
        ),
    )(*operands)


def scatter_jobs(shapes):
    order = [(4, 0, 96), (6, 0, None), (2, 0, None), (4, 96, 96), (3, 0, None), (5, 0, None)]
    order += [(4, 192, 96)] + [(at, 0, None) for at in (1, 7, 0, 8, 9)]
    return [(at, row, size or shapes[at][0], at == 4) for at, row, size in order]


def scatter_kernel(jobs, *refs):
    single = jnp.float32
    count = len(jobs)
    terms, refs = refs[:10], refs[10:]
    outs, refs = refs[:10], refs[10:]
    own, refs = refs[:count], refs[count:]
    landed, refs = refs[:count], refs[count:]
    partial, refs = refs[:count], refs[count:]
    final, refs = refs[:count], refs[count:]
    own_sem, send_one, receive_one, send_two, receive_two = refs
    slab = lax.axis_index("slab")
    y, z = slab // 4, slab % 4
    barrier = pltpu.get_barrier_semaphore()

    def peer(along_y, step):
        if along_y:
            spot = (y + step) % 4
            return spot, spot * 4 + z
        spot = (z + step) % 4
        return spot, y * 4 + spot

    for along_y in (True, False):
        for step in (1, 2, 3):
            pl.semaphore_signal(
                barrier,
                inc=1,
                device_id={"slab": peer(along_y, step)[1]},
                device_id_type=MESH,
            )
    pl.semaphore_wait(barrier, 6)

    def group(job, spot):
        at, row, size, along_y = jobs[job]
        rows = pl.ds(row, size)
        if along_y:
            return terms[at].at[spot, :, rows]
        return terms[at].at[:, spot, rows]

    def keep(job):
        return pltpu.make_async_copy(
            group(job, y if jobs[job][3] else z), own[job], own_sem.at[job]
        )

    def first(job, step):
        spot, target = peer(jobs[job][3], step)
        return pltpu.make_async_remote_copy(
            src_ref=group(job, spot),
            dst_ref=landed[job].at[step - 1],
            send_sem=send_one.at[job, step - 1],
            recv_sem=receive_one.at[job, step - 1],
            device_id={"slab": target},
            device_id_type=MESH,
        )

    def second(job, step):
        spot, target = peer(not jobs[job][3], step)
        return pltpu.make_async_remote_copy(
            src_ref=partial[job].at[spot],
            dst_ref=final[job].at[step - 1],
            send_sem=send_two.at[job, step - 1],
            recv_sem=receive_two.at[job, step - 1],
            device_id={"slab": target},
            device_id_type=MESH,
        )

    for job in range(count):
        for step in (2, 1, 3):
            first(job, step).start()
        keep(job).start()
    for job in range(count):
        keep(job).wait()
        for step in (1, 2, 3):
            first(job, step).wait_recv()

        def add(spot, carry, job=job):
            total = own[job][spot].astype(single)
            for step in range(3):
                total = total + landed[job][step, spot].astype(single)
            partial[job][spot] = total.astype(jnp.bfloat16)
            return carry

        lax.fori_loop(0, 4, add, 0)
        for step in (2, 1, 3):
            second(job, step).start()
    for job in range(count):
        at, row, size, along_y = jobs[job]
        for step in (1, 2, 3):
            second(job, step).wait_recv()
        total = partial[job][z if along_y else y].astype(single)
        for step in range(3):
            total = total + final[job][step].astype(single)
        outs[at][pl.ds(row, size), :] = total
    for job in range(count):
        for step in (1, 2, 3):
            first(job, step).wait_send()
            second(job, step).wait_send()


def hand_over(*refs):
    count = len(refs) // 2
    semaphores = refs[-1]
    copies = [
        pltpu.make_async_copy(refs[k], refs[count + k], semaphores.at[k]) for k in range(count)
    ]
    for copy in copies:
        copy.start()
    for copy in copies:
        copy.wait()


def scatter_sums(terms):
    bfloat = jnp.bfloat16
    shapes = [(term.shape[0] // 16, term.shape[1]) for term in terms]
    jobs = scatter_jobs(shapes)
    blocks = [(size, shapes[at][1]) for at, _, size, _ in jobs]
    scratch = [pltpu.VMEM((4, *block), bfloat) for block in blocks]
    scratch += [pltpu.VMEM((3, 4, *block), bfloat) for block in blocks]
    scratch += [pltpu.VMEM((4, *block), bfloat) for block in blocks]
    scratch += [pltpu.VMEM((3, *block), bfloat) for block in blocks]
    scratch += [pltpu.SemaphoreType.DMA((len(jobs),))]
    scratch += [pltpu.SemaphoreType.DMA((len(jobs), 3)) for _ in range(4)]
    sums = pl.pallas_call(
        functools.partial(scatter_kernel, jobs),
        out_shape=[jax.ShapeDtypeStruct(shape, jnp.float32) for shape in shapes],
        in_specs=[pl.BlockSpec(memory_space=pl.ANY)] * len(terms),
        out_specs=[pl.BlockSpec(memory_space=pltpu.VMEM)] * len(terms),
        scratch_shapes=scratch,
        compiler_params=pltpu.CompilerParams(
            collective_id=1, has_side_effects=True, vmem_limit_bytes=67043328
        ),
        cost_estimate=pl.CostEstimate(
            flops=2_000_000_000, bytes_accessed=30_000_000, transcendentals=0
        ),
    )(*[term.reshape(4, 4, *shape) for term, shape in zip(terms, shapes)])
    return pl.pallas_call(
        hand_over,
        out_shape=[jax.ShapeDtypeStruct(shape, jnp.float32) for shape in shapes],
        in_specs=[pl.BlockSpec(memory_space=pltpu.VMEM)] * len(sums),
        out_specs=[pl.BlockSpec(memory_space=pl.ANY)] * len(sums),
        scratch_shapes=[pltpu.SemaphoreType.DMA((len(sums),))],
        compiler_params=pltpu.CompilerParams(vmem_limit_bytes=67043328),
    )(*sums)


def repeat(bound, body, unroll):
    def step(index, carry):
        body(index)
        return carry

    lax.fori_loop(0, bound, step, 0, unroll=unroll)


def cell_mask(cells, block):
    row = cells[pl.ds(block, 1), :]
    place = lax.broadcasted_iota(jnp.int32, (TILE, row.shape[1]), 0)
    return (jnp.broadcast_to(row, place.shape) == place).astype(jnp.bfloat16)


def deposit_kernel(slots, cells, features, out):
    zero = jnp.zeros((TILE, TILE), jnp.bfloat16)

    def clear(slot):
        out[slot] = zero

    repeat(out.shape[0], clear, 8)

    def deposit(block):
        value = jnp.dot(
            cell_mask(cells, block), features[block], preferred_element_type=jnp.float32
        )
        out[slots[block]] = value.astype(jnp.bfloat16)

    repeat(features.shape[0], deposit, 8)


def splat_kernel(tiles, incoming, base, out, canvas):
    zero = jnp.zeros((TILE, TILE), jnp.float32)

    def clear(tile):
        canvas[tile] = zero

    repeat(canvas.shape[0], clear, 3)

    def add(slot):
        tile = tiles[slot]
        canvas[tile] = canvas[tile] + incoming[slot].astype(jnp.float32)

    repeat(incoming.shape[0], add, 4)

    def finish(row):
        for k in range(4):
            for half in range(2):
                cells = slice(k * 64 + half * 32, k * 64 + half * 32 + 32)
                total = base[row, cells].astype(jnp.float32)
                total = total + canvas[2 * row + half, k * 32 : k * 32 + 32]
                out[row, cells] = total.astype(jnp.bfloat16)

    repeat(out.shape[0], finish, 2)


def pick_kernel(tiles, gradient, out):
    def pick(slot):
        tile = tiles[slot]
        row, half = lax.div(tile, 2), lax.rem(tile, 2)
        for k in range(4):
            cells = pl.ds(pl.multiple_of(k * 64 + half * 32, 32), 32)
            out[slot, k * 32 : k * 32 + 32] = gradient[row, cells]

    repeat(out.shape[0], pick, 4)


def camera_kernel(slots, cells, returned, out):
    def camera(block):
        out[block] = outer(cell_mask(cells, block), returned[slots[block]]).astype(jnp.bfloat16)

    repeat(out.shape[0], camera, 8)


def local_call(kernel, shape, operands, scratch=()):
    vector = pl.BlockSpec(memory_space=pltpu.VMEM)
    return pl.pallas_call(
        kernel,
        out_shape=jax.ShapeDtypeStruct(shape, jnp.bfloat16),
        in_specs=[pl.BlockSpec(memory_space=pltpu.SMEM)] + [vector] * (len(operands) - 1),
        out_specs=vector,
        scratch_shapes=scratch,
        compiler_params=pltpu.CompilerParams(vmem_limit_bytes=40000000),
        cost_estimate=pl.CostEstimate(
            flops=400_000_000, bytes_accessed=8_000_000, transcendentals=0
        ),
    )(*operands)


def by_parity(field):
    rows, across, channels = field.shape
    return (
        field.reshape(rows, across // 4, 2, 2, channels)
        .transpose(0, 3, 2, 1, 4)
        .reshape(rows, across, channels)
    )


def body(
    camera_features,
    cell_index,
    owner_device,
    owner_tile,
    base_map,
    targets,
    fine_conv,
    fine_down,
    middle_conv,
    middle_down,
    coarse_conv,
    coarse_up,
    middle_merge,
    middle_up,
    fine_merge,
    head_weight,
):
    single = jnp.float32
    bfloat = jnp.bfloat16
    device = lax.axis_index("slab")
    devices = lax.axis_size("slab")
    height, across, channels = base_map.shape
    slot_count = devices * CAP
    tile_count = height * across // TILE
    owners = owner_device[:, 0]
    everyone = owners.shape[0]
    choose = (owners[:, None] == jnp.arange(devices, dtype=jnp.int32)[None, :]).astype(jnp.int32)
    grouped = choose.reshape(devices, BLK_DEV, devices)
    earlier = (jnp.cumsum(grouped, axis=1) - grouped).reshape(everyone, devices)
    ranking = jnp.sum(earlier * choose, axis=1)
    sources = jnp.arange(everyone, dtype=jnp.int32) // BLK_DEV
    slot_number = owners * CAP + ranking
    local_slot = lax.dynamic_slice_in_dim(slot_number, device * BLK_DEV, BLK_DEV)
    slot_range = jnp.arange(slot_count, dtype=jnp.int32)
    arrival = sources * CAP + ranking
    receive_map = ((arrival[None, :] == slot_range[:, None]) & (owners[None, :] == device)).astype(
        jnp.int32
    )
    received = jnp.sum(receive_map, axis=1)
    slot_tiles = jnp.sum(receive_map * owner_tile[None, :], axis=1)
    landing_tiles = jnp.where(received > 0, slot_tiles, tile_count)
    local_cells = lax.dynamic_slice_in_dim(cell_index, device * BLK_DEV, BLK_DEV)
    local_cells = local_cells % 2 * 64 + local_cells // 2 % 2 * 32 + local_cells // 4
    wire = (devices, CAP * TILE, channels)
    outgoing = local_call(
        deposit_kernel,
        (slot_count, TILE, channels),
        (local_slot, local_cells, camera_features),
    )
    incoming = lax.all_to_all(
        outgoing.reshape(wire), "slab", split_axis=0, concat_axis=0, tiled=True
    ).reshape(slot_count, TILE, channels)
    level_zero = local_call(
        splat_kernel,
        (height, across, channels),
        (landing_tiles, incoming, by_parity(base_map)),
        [pltpu.VMEM((tile_count + 1, TILE, channels), single)],
    )
    level_zero_grad, losses, *terms = unet(
        level_zero,
        by_parity(targets),
        fine_conv,
        fine_down,
        middle_conv,
        middle_down,
        coarse_conv,
        coarse_up,
        middle_merge,
        middle_up,
        fine_merge,
        head_weight,
        flipped(fine_conv),
        flipped(middle_conv),
        flipped(coarse_conv),
        flipped(middle_merge),
        flipped(fine_merge),
    )
    row_loss = jnp.sum(losses[:, 0, :], axis=1) / (across * K)
    slot_grad = local_call(
        pick_kernel, (slot_count, TILE, channels), (slot_tiles, level_zero_grad)
    )
    returned = lax.all_to_all(
        slot_grad.reshape(wire), "slab", split_axis=0, concat_axis=0, tiled=True
    ).reshape(slot_count, TILE, channels)
    camera_grad = local_call(
        camera_kernel, camera_features.shape, (local_slot, local_cells, returned)
    )
    sums = scatter_sums(terms)
    return (camera_grad, row_loss, *sums)


def solution(mesh):
    step = jax.shard_map(
        body,
        mesh=mesh,
        in_specs=(
            P(("scene", "slab"), None, None),
            P("scene", None),
            P("scene", None),
            P("scene"),
            P(("scene", "slab"), None, None),
            P(("scene", "slab"), None, None),
            P(),
            P(),
            P(),
            P(),
            P(),
            P(),
            P(),
            P(),
            P(),
            P(),
        ),
        out_specs=(
            P(("scene", "slab"), None, None),
            P(("scene", "slab")),
            P(("scene", "slab"), None),
            P(("scene", "slab"), None),
            P(("scene", "slab"), None),
            P(("scene", "slab"), None),
            P(("scene", "slab"), None),
            P(("scene", "slab"), None),
            P(("scene", "slab"), None),
            P(("scene", "slab"), None),
            P(("scene", "slab"), None),
            P(("scene", "slab"), None),
        ),
        check_vma=False,
    )
    return step
```

```python
import functools

import jax
import jax.numpy as jnp
from jax import lax
from jax.experimental import pallas as pl
from jax.experimental.pallas import tpu as pltpu
from jax.sharding import PartitionSpec as P

BLK_DEV = 64
C1 = 256
C2 = 512
K = 128
TILE = 128
CAP = 8
MESH = pl.DeviceIdType.MESH


loss_weight = 0.0625


def flipped(weight):
    inward = weight.shape[0] // 9
    return weight.reshape(9, inward, -1)[::-1].transpose(0, 2, 1).reshape(-1, inward)


def silu_slope(signal):
    logistic = jax.nn.sigmoid(signal)
    return logistic * (1.0 + signal * (1.0 - logistic))


def outer(former, latter):
    return lax.dot_general(
        former, latter, (((0,), (0,)), ((), ())), preferred_element_type=jnp.float32
    )


def backward(former, latter):
    return lax.dot_general(
        former, latter, (((1,), (1,)), ((), ())), preferred_element_type=jnp.float32
    )


def lower_rows(block):
    moved = pltpu.roll(block.astype(jnp.float32), 1, 0)
    place = lax.broadcasted_iota(jnp.int32, moved.shape, 0)
    return jnp.where(place == 0, 0.0, moved).astype(block.dtype)


def upper_rows(block):
    length = block.shape[0]
    moved = pltpu.roll(block.astype(jnp.float32), length - 1, 0)
    place = lax.broadcasted_iota(jnp.int32, moved.shape, 0)
    return jnp.where(place == length - 1, 0.0, moved).astype(block.dtype)


def shifted_pair(row):
    span = 64
    blocks = [row[at : at + span] for at in range(0, row.shape[0], span)]
    if len(blocks) == 1:
        return lower_rows(row), upper_rows(row)
    if len(blocks) == 2:
        left = [lower_rows(blocks[1]), blocks[0]]
        right = [blocks[1], upper_rows(blocks[0])]
    else:
        left = [lower_rows(blocks[3]), blocks[2], blocks[0], blocks[1]]
        right = [blocks[2], blocks[3], blocks[1], upper_rows(blocks[0])]
    return jnp.concatenate(left, axis=0), jnp.concatenate(right, axis=0)


def window(start, size):
    if isinstance(start, int):
        return pl.ds(start, size)
    return pl.ds(pl.multiple_of(start, size if size < 64 else 64), size)


def put_row(field, at, row):
    span, channels = row.shape
    left, right = shifted_pair(row)
    rows = window(at * span, span)
    field[rows, 0:channels] = left
    field[rows, channels : 2 * channels] = row
    field[rows, 2 * channels : 3 * channels] = right


def tap_rows(field, first, count, span):
    return jnp.concatenate(
        [field[window((first + step) * span, count * span), :] for step in range(3)], axis=1
    )


def times(former, latter):
    return jnp.dot(former, latter, preferred_element_type=jnp.float32)


def unet_kernel(*refs):
    loads = [
        pltpu.make_async_copy(refs[2 + k], refs[k - 16], refs[-1].at[k]) for k in range(15)
    ]
    refs = refs[:2] + refs[-16:-1] + refs[17:-16]
    for k in (0, 1, 2, 3, 4, 5, 6, 7, 8, 9, 14, 13, 12, 11, 10):
        loads[k].start()
    (
        zero_ref, labels_ref, fine_conv, fine_down, middle_conv, middle_down, coarse_conv,
        coarse_up, middle_merge, middle_up, fine_merge, head, flip_fine, flip_middle,
        flip_coarse, flip_merge, flip_top,
        zero_grad, loss_ref, g_fine, g_fine_down, g_middle, g_middle_down, g_coarse,
        g_coarse_up, g_merge, g_up, g_top, g_head,
        field_zero, field_top, field_fine, field_one, field_merge, field_middle, field_two,
        field_coarse, pre_fine, hid_fine, pre_middle, hid_middle, pre_coarse, hid_coarse,
        pre_merge, out_middle, grad_fine, grad_middle, grad_one, sum_fine, sum_middle, sum_head,
        edges_fine, edges_middle, edges_coarse, halo_fine, halo_middle, halo_coarse,
        send_sem, receive_sem,
    ) = refs
    bfloat, single = jnp.bfloat16, jnp.float32
    slab = lax.axis_index("slab")
    last = lax.axis_size("slab") - 1
    barrier = pltpu.get_barrier_semaphore()

    for step in (1, last):
        pl.semaphore_signal(
            barrier,
            inc=1,
            device_id={"slab": lax.rem(slab + step, last + 1)},
            device_id_type=MESH,
        )
    pl.semaphore_wait(barrier, 2)

    def edge_copy(source, halo, exchange, slot, way):
        return pltpu.make_async_remote_copy(
            src_ref=source,
            dst_ref=halo.at[slot, way],
            send_sem=send_sem.at[exchange, way],
            recv_sem=receive_sem.at[exchange, way],
            device_id={"slab": slab + (1 if way == 0 else -1)},
            device_id_type=MESH,
        )

    started = []

    def send_edges(top, bottom, halo, exchange, slot):
        started.append((top, bottom, halo, exchange, slot))

        @pl.when(slab < last)
        def _():
            edge_copy(bottom, halo, exchange, slot, 0).start()

        @pl.when(slab > 0)
        def _():
            edge_copy(top, halo, exchange, slot, 1).start()

    def take_edges(field, height):
        top, bottom, halo, exchange, slot = started[-1]

        @pl.when(slab > 0)
        def _():
            edge_copy(bottom, halo, exchange, slot, 0).wait_recv()

        @pl.when(slab == 0)
        def _():
            halo[slot, 0] = jnp.zeros(halo.shape[2:], halo.dtype)

        @pl.when(slab < last)
        def _():
            edge_copy(top, halo, exchange, slot, 1).wait_recv()

        @pl.when(slab == last)
        def _():
            halo[slot, 1] = jnp.zeros(halo.shape[2:], halo.dtype)

        put_row(field, 0, halo[slot, 0])
        put_row(field, height + 1, halo[slot, 1])

    def each(first, bound, body):
        def step(index, carry):
            body(index)
            return carry

        lax.fori_loop(first, bound, step, 0)

    def fine_rows(handle, inner, outer_):
        if inner:
            each(1, 7, handle)
        if outer_:
            each(0, 2, lambda index: handle(index * 7))

    def middle_rows(handle, inner, outer_):
        if inner:
            each(1, 3, handle)
        if outer_:
            each(0, 2, lambda index: handle(index * 3))

    quads = [(0, 0), (0, 1), (1, 0), (1, 1)]

    send_edges(zero_ref.at[0], zero_ref.at[15], halo_fine, 0, 0)
    each(0, 16, lambda row: put_row(field_zero, row + 1, zero_ref[row]))

    def fine_step(at):
        pre = times(tap_rows(field_zero, 2 * at, 2, 256), fine_conv[...])
        rows = window(at * 128, 128)
        for k in range(4):
            part = pre[k * 128 : (k + 1) * 128]
            pre_fine[rows, k * 128 : (k + 1) * 128] = part
            hid_fine[rows, k * 128 : (k + 1) * 128] = jax.nn.silu(part).astype(bfloat)

    loads[0].wait()
    fine_rows(fine_step, True, False)
    take_edges(field_zero, 16)
    fine_rows(fine_step, False, True)

    def one_step(at):
        value = times(hid_fine[window(at * 256, 256), :], fine_down[...]).astype(bfloat)
        for k in range(2):
            put_row(field_one, 2 * at + k + 1, value[k * 128 : (k + 1) * 128])

    def middle_edges(field, slot):
        edges_middle[slot, 0] = field[pl.ds(128, 128), 256:512]
        edges_middle[slot, 1] = field[pl.ds(8 * 128, 128), 256:512]

    loads[1].wait()
    middle_rows(one_step, False, True)
    middle_edges(field_one, 0)
    send_edges(edges_middle.at[0, 0], edges_middle.at[0, 1], halo_middle, 1, 0)
    middle_rows(one_step, True, False)

    def middle_step(at):
        pre = times(tap_rows(field_one, 2 * at, 2, 128), middle_conv[...])
        rows = window(at * 64, 64)
        for k in range(4):
            part = pre[k * 64 : (k + 1) * 64]
            pre_middle[rows, k * 256 : (k + 1) * 256] = part
            hid_middle[rows, k * 256 : (k + 1) * 256] = jax.nn.silu(part).astype(bfloat)

    loads[2].wait()
    middle_rows(middle_step, True, False)
    take_edges(field_one, 8)
    middle_rows(middle_step, False, True)

    def spread_coarse(field, value, slot, exchange):
        for row in range(4):
            put_row(field, row + 1, value[row * 64 : (row + 1) * 64])
        edges_coarse[slot, 0] = value[0:64]
        edges_coarse[slot, 1] = value[192:256]
        send_edges(edges_coarse.at[slot, 0], edges_coarse.at[slot, 1], halo_coarse, exchange, slot)

    def coarse_part(field, weight, step):
        return times(
            field[window(step * 64, 256), :], weight[window(step * 1536, 1536), :]
        )

    loads[3].wait()
    value = times(hid_middle[...], middle_down[...]).astype(bfloat)
    spread_coarse(field_two, value, 0, 2)
    loads[4].wait()
    pre_coarse[...] = coarse_part(field_two, coarse_conv, 1)
    take_edges(field_two, 4)

    def coarse_step(index):
        pre_coarse[...] += coarse_part(field_two, coarse_conv, 2 * index)

    each(0, 2, coarse_step)
    hid_coarse[...] = jax.nn.silu(pre_coarse[...]).astype(bfloat)

    def join_middle(at):
        rows = window(at * 64, 64)
        total = times(hid_coarse[rows, :], coarse_up[...]) + hid_middle[rows, :].astype(single)
        total = total.astype(bfloat)
        for i in range(2):
            row = jnp.concatenate(
                [total[:, (2 * i + j) * 256 : (2 * i + j + 1) * 256] for j in range(2)], axis=0
            )
            put_row(field_merge, 2 * at + i + 1, row)

    loads[5].wait()
    middle_rows(join_middle, False, True)
    middle_edges(field_merge, 1)
    send_edges(edges_middle.at[1, 0], edges_middle.at[1, 1], halo_middle, 3, 1)
    middle_rows(join_middle, True, False)

    def merge_step(at):
        pre = times(tap_rows(field_merge, 2 * at, 2, 128), middle_merge[...])
        rows = window(at * 256, 256)
        pre_merge[rows, :] = pre
        out_middle[rows, :] = jax.nn.silu(pre).astype(bfloat)

    loads[6].wait()
    middle_rows(merge_step, True, False)
    take_edges(field_merge, 8)
    middle_rows(merge_step, False, True)

    def join_fine(at):
        rows = window(at * 128, 128)
        total = times(out_middle[rows, :], middle_up[...]) + hid_fine[rows, :].astype(single)
        total = total.astype(bfloat)
        for i in range(2):
            row = jnp.concatenate(
                [total[:, (2 * i + j) * 128 : (2 * i + j + 1) * 128] for j in range(2)], axis=0
            )
            put_row(field_top, 2 * at + i + 1, row)

    def fine_edges(field, slot):
        edges_fine[slot, 0] = field[pl.ds(256, 256), 128:256]
        edges_fine[slot, 1] = field[pl.ds(16 * 256, 256), 128:256]

    loads[7].wait()
    fine_rows(join_fine, False, True)
    fine_edges(field_top, 0)
    send_edges(edges_fine.at[0, 0], edges_fine.at[0, 1], halo_fine, 4, 1)
    fine_rows(join_fine, True, False)
    sum_head[...] = jnp.zeros_like(sum_head)

    def top_step(at):
        pre = times(tap_rows(field_top, 2 * at, 2, 256), fine_merge[...])
        logistic = jax.nn.sigmoid(pre)
        out_fine = (pre * logistic).astype(bfloat)
        logits = times(out_fine, head[...])
        for i in range(2):
            row = logits[i * 256 : (i + 1) * 256]
            labels = labels_ref[2 * at + i].astype(single)
            spread = jnp.maximum(row, 0.0) + jnp.log1p(jnp.exp(-jnp.abs(row)))
            penalty = jnp.sum(spread - labels * row, axis=0, keepdims=True)
            loss_ref[2 * at + i] = jnp.broadcast_to(penalty, (8, 128))
            slope = ((jax.nn.sigmoid(row) - labels) * loss_weight).astype(bfloat)
            one = slice(i * 256, (i + 1) * 256)
            sum_head[...] += outer(out_fine[one], slope)
            level = logistic[one]
            down = backward(slope, head[...]) * (level * (1.0 + pre[one] * (1.0 - level)))
            put_row(field_fine, 2 * at + i + 1, down.astype(bfloat))

    loads[8].wait()
    loads[9].wait()
    fine_rows(top_step, True, False)
    take_edges(field_top, 16)
    fine_rows(top_step, False, True)
    g_head[...] = sum_head[...].astype(bfloat)
    fine_edges(field_fine, 1)
    send_edges(edges_fine.at[1, 0], edges_fine.at[1, 1], halo_fine, 5, 2)

    def fine_weight(field, grad_out):
        sum_fine[...] = jnp.zeros_like(sum_fine)

        def step(at):
            back = field_fine[window((2 * at + 1) * 256, 512), 128:256]
            sum_fine[...] += outer(back, tap_rows(field, 2 * at, 2, 256))

        each(0, 8, step)
        for k in range(9):
            part = sum_fine[:, k * 128 : (k + 1) * 128]
            grad_out[pl.ds(k * 128, 128), :] = part.T.astype(bfloat)

    fine_weight(field_top, g_top)
    take_edges(field_fine, 16)

    def grad_fine_step(at):
        value = times(tap_rows(field_fine, 2 * at, 2, 256), flip_top[...]).astype(bfloat)
        rows = window(at * 128, 128)
        for k in range(4):
            grad_fine[rows, k * 128 : (k + 1) * 128] = value[k * 128 : (k + 1) * 128]

    loads[14].wait()
    each(0, 8, grad_fine_step)

    def back_merge_step(at):
        rows = window(at * 256, 256)
        value = backward(grad_fine[rows, :], middle_up[...]) * silu_slope(pre_merge[rows, :])
        value = value.astype(bfloat)
        for k in range(2):
            put_row(field_middle, 2 * at + k + 1, value[k * 128 : (k + 1) * 128])

    each(0, 4, back_merge_step)
    middle_edges(field_middle, 2)
    send_edges(edges_middle.at[2, 0], edges_middle.at[2, 1], halo_middle, 6, 2)
    g_up[...] = outer(out_middle[...], grad_fine[...]).astype(bfloat)

    def middle_weight(field, grad_out):
        for part in range(3):
            total = jnp.zeros((256, 768), single)
            back = field_middle[pl.ds(128, 1024), 256:512]
            taps = field[pl.ds(part * 128, 1024), :]
            total = outer(back, taps)
            for k in range(3):
                grad_out[pl.ds(part * 768 + k * 256, 256), :] = (
                    total[:, k * 256 : (k + 1) * 256].T.astype(bfloat)
                )

    middle_weight(field_merge, g_merge)
    take_edges(field_middle, 8)

    def grad_middle_step(at):
        value = times(tap_rows(field_middle, 2 * at, 2, 128), flip_merge[...]).astype(bfloat)
        rows = window(at * 64, 64)
        for k in range(4):
            grad_middle[rows, k * 256 : (k + 1) * 256] = value[k * 64 : (k + 1) * 64]

    loads[13].wait()
    each(0, 4, grad_middle_step)

    value = backward(grad_middle[...], coarse_up[...]) * silu_slope(pre_coarse[...])
    spread_coarse(field_coarse, value.astype(bfloat), 1, 7)
    g_coarse_up[...] = outer(hid_coarse[...], grad_middle[...]).astype(bfloat)

    def coarse_weight(step):
        back = field_coarse[pl.ds(64, 256), 512:1024]
        total = outer(field_two[window(step * 64, 256), :], back)
        g_coarse[window(step * 1536, 1536), :] = total.astype(bfloat)

    each(0, 3, coarse_weight)
    take_edges(field_coarse, 4)
    loads[12].wait()
    pre_coarse[...] = coarse_part(field_coarse, flip_coarse, 1)

    def coarse_back(index):
        pre_coarse[...] += coarse_part(field_coarse, flip_coarse, 2 * index)

    each(0, 2, coarse_back)
    value = pre_coarse[...].astype(bfloat)

    hid_coarse[...] = value

    def back_middle_step(at):
        rows = window(at * 64, 64)
        total = backward(hid_coarse[rows, :], middle_down[...]) + grad_middle[rows, :].astype(single)
        total = (total * silu_slope(pre_middle[rows, :])).astype(bfloat)
        for i in range(2):
            row = jnp.concatenate(
                [total[:, (2 * i + j) * 256 : (2 * i + j + 1) * 256] for j in range(2)], axis=0
            )
            put_row(field_middle, 2 * at + i + 1, row)

    each(0, 4, back_middle_step)
    middle_edges(field_middle, 3)
    send_edges(edges_middle.at[3, 0], edges_middle.at[3, 1], halo_middle, 8, 3)
    g_middle_down[...] = outer(hid_middle[...], hid_coarse[...]).astype(bfloat)
    middle_weight(field_one, g_middle)
    take_edges(field_middle, 8)

    def grad_one_step(at):
        value = times(tap_rows(field_middle, 2 * at, 2, 128), flip_middle[...]).astype(bfloat)
        grad_one[window(at * 256, 256), :] = value

    loads[11].wait()
    each(0, 4, grad_one_step)

    def back_fine_step(at):
        rows = window(at * 128, 128)
        total = backward(grad_one[rows, :], fine_down[...]) + grad_fine[rows, :].astype(single)
        total = (total * silu_slope(pre_fine[rows, :])).astype(bfloat)
        for i in range(2):
            row = jnp.concatenate(
                [total[:, (2 * i + j) * 128 : (2 * i + j + 1) * 128] for j in range(2)], axis=0
            )
            put_row(field_fine, 2 * at + i + 1, row)

    each(0, 8, back_fine_step)
    fine_edges(field_fine, 2)
    send_edges(edges_fine.at[2, 0], edges_fine.at[2, 1], halo_fine, 9, 3)
    g_fine_down[...] = outer(hid_fine[...], grad_one[...]).astype(bfloat)
    fine_weight(field_zero, g_fine)
    take_edges(field_fine, 16)

    def zero_step(at):
        value = times(tap_rows(field_fine, 2 * at, 2, 256), flip_fine[...]).astype(bfloat)
        for i in range(2):
            zero_grad[2 * at + i] = value[i * 256 : (i + 1) * 256]

    loads[10].wait()
    each(0, 8, zero_step)

    for top, bottom, halo, exchange, slot in started:

        @pl.when(slab < last)
        def _():
            edge_copy(bottom, halo, exchange, slot, 0).wait_send()

        @pl.when(slab > 0)
        def _():
            edge_copy(top, halo, exchange, slot, 1).wait_send()


def unet(*operands):
    bfloat, single = jnp.bfloat16, jnp.float32
    shapes = [
        ((16, 256, 128), bfloat), ((16, 8, 128), single), ((1152, 128), bfloat),
        ((512, 256), bfloat), ((2304, 256), bfloat), ((1024, 512), bfloat),
        ((4608, 512), bfloat), ((512, 1024), bfloat), ((2304, 256), bfloat),
        ((256, 512), bfloat), ((1152, 128), bfloat), ((128, 128), bfloat),
    ]
    scratch = [
        ((18 * 256, 384), bfloat), ((18 * 256, 384), bfloat), ((18 * 256, 384), bfloat),
        ((10 * 128, 768), bfloat), ((10 * 128, 768), bfloat), ((10 * 128, 768), bfloat),
        ((6 * 64, 1536), bfloat), ((6 * 64, 1536), bfloat),
        ((1024, 512), single), ((1024, 512), bfloat),
        ((256, 1024), single), ((256, 1024), bfloat),
        ((256, 512), single), ((256, 512), bfloat),
        ((1024, 256), single), ((1024, 256), bfloat),
        ((1024, 512), bfloat), ((256, 1024), bfloat), ((1024, 256), bfloat),
        ((128, 1152), single), ((8, 128), single), ((128, 128), single),
        ((3, 2, 256, 128), bfloat), ((4, 2, 128, 256), bfloat), ((2, 2, 64, 512), bfloat),
        ((4, 2, 256, 128), bfloat), ((4, 2, 128, 256), bfloat), ((2, 2, 64, 512), bfloat),
    ]
    return pl.pallas_call(
        unet_kernel,
        out_shape=[jax.ShapeDtypeStruct(*leaf) for leaf in shapes],
        in_specs=[pl.BlockSpec(memory_space=pltpu.VMEM)] * 2
        + [pl.BlockSpec(memory_space=pl.ANY)] * 15,
        out_specs=[pl.BlockSpec(memory_space=pltpu.VMEM)] * len(shapes),
        scratch_shapes=[pltpu.VMEM(*leaf) for leaf in scratch]
        + [pltpu.SemaphoreType.DMA((10, 2)), pltpu.SemaphoreType.DMA((10, 2))]
        + [pltpu.VMEM(weight.shape, bfloat) for weight in operands[2:]]
        + [pltpu.SemaphoreType.DMA((15,))],
        compiler_params=pltpu.CompilerParams(
            collective_id=0, has_side_effects=True, vmem_limit_bytes=67043328
        ),
        cost_estimate=pl.CostEstimate(
            flops=24_000_000_000, bytes_accessed=40_000_000, transcendentals=4_000_000
        ),
    )(*operands)


def scatter_jobs(shapes):
    order = [(4, 0, 96), (6, 0, None), (2, 0, None), (4, 96, 96), (3, 0, None), (5, 0, None)]
    order += [(4, 192, 96)] + [(at, 0, None) for at in (1, 7, 0, 8, 9)]
    return [(at, row, size or shapes[at][0], at == 4) for at, row, size in order]


def scatter_kernel(jobs, *refs):
    single = jnp.float32
    count = len(jobs)
    terms, refs = refs[:10], refs[10:]
    outs, refs = refs[:10], refs[10:]
    own, refs = refs[:count], refs[count:]
    landed, refs = refs[:count], refs[count:]
    partial, refs = refs[:count], refs[count:]
    final, refs = refs[:count], refs[count:]
    own_sem, send_one, receive_one, send_two, receive_two = refs
    slab = lax.axis_index("slab")
    y, z = slab // 4, slab % 4
    barrier = pltpu.get_barrier_semaphore()

    def peer(along_y, step):
        if along_y:
            spot = (y + step) % 4
            return spot, spot * 4 + z
        spot = (z + step) % 4
        return spot, y * 4 + spot

    for along_y in (True, False):
        for step in (1, 2, 3):
            pl.semaphore_signal(
                barrier,
                inc=1,
                device_id={"slab": peer(along_y, step)[1]},
                device_id_type=MESH,
            )
    pl.semaphore_wait(barrier, 6)

    def group(job, spot):
        at, row, size, along_y = jobs[job]
        rows = pl.ds(row, size)
        if along_y:
            return terms[at].at[spot, :, rows]
        return terms[at].at[:, spot, rows]

    def keep(job):
        return pltpu.make_async_copy(
            group(job, y if jobs[job][3] else z), own[job], own_sem.at[job]
        )

    def first(job, step):
        spot, target = peer(jobs[job][3], step)
        return pltpu.make_async_remote_copy(
            src_ref=group(job, spot),
            dst_ref=landed[job].at[step - 1],
            send_sem=send_one.at[job, step - 1],
            recv_sem=receive_one.at[job, step - 1],
            device_id={"slab": target},
            device_id_type=MESH,
        )

    def second(job, step):
        spot, target = peer(not jobs[job][3], step)
        return pltpu.make_async_remote_copy(
            src_ref=partial[job].at[spot],
            dst_ref=final[job].at[step - 1],
            send_sem=send_two.at[job, step - 1],
            recv_sem=receive_two.at[job, step - 1],
            device_id={"slab": target},
            device_id_type=MESH,
        )

    for job in range(count):
        for step in (2, 1, 3):
            first(job, step).start()
        keep(job).start()
    for job in range(count):
        keep(job).wait()
        for step in (1, 2, 3):
            first(job, step).wait_recv()

        def add(spot, carry, job=job):
            total = own[job][spot].astype(single)
            for step in range(3):
                total = total + landed[job][step, spot].astype(single)
            partial[job][spot] = total.astype(jnp.bfloat16)
            return carry

        lax.fori_loop(0, 4, add, 0)
        for step in (2, 1, 3):
            second(job, step).start()
    for job in range(count):
        at, row, size, along_y = jobs[job]
        for step in (1, 2, 3):
            second(job, step).wait_recv()
        total = partial[job][z if along_y else y].astype(single)
        for step in range(3):
            total = total + final[job][step].astype(single)
        outs[at][pl.ds(row, size), :] = total
    for job in range(count):
        for step in (1, 2, 3):
            first(job, step).wait_send()
            second(job, step).wait_send()


def hand_over(*refs):
    count = len(refs) // 2
    semaphores = refs[-1]
    copies = [
        pltpu.make_async_copy(refs[k], refs[count + k], semaphores.at[k]) for k in range(count)
    ]
    for copy in copies:
        copy.start()
    for copy in copies:
        copy.wait()


def scatter_sums(terms):
    bfloat = jnp.bfloat16
    shapes = [(term.shape[0] // 16, term.shape[1]) for term in terms]
    jobs = scatter_jobs(shapes)
    blocks = [(size, shapes[at][1]) for at, _, size, _ in jobs]
    scratch = [pltpu.VMEM((4, *block), bfloat) for block in blocks]
    scratch += [pltpu.VMEM((3, 4, *block), bfloat) for block in blocks]
    scratch += [pltpu.VMEM((4, *block), bfloat) for block in blocks]
    scratch += [pltpu.VMEM((3, *block), bfloat) for block in blocks]
    scratch += [pltpu.SemaphoreType.DMA((len(jobs),))]
    scratch += [pltpu.SemaphoreType.DMA((len(jobs), 3)) for _ in range(4)]
    sums = pl.pallas_call(
        functools.partial(scatter_kernel, jobs),
        out_shape=[jax.ShapeDtypeStruct(shape, jnp.float32) for shape in shapes],
        in_specs=[pl.BlockSpec(memory_space=pl.ANY)] * len(terms),
        out_specs=[pl.BlockSpec(memory_space=pltpu.VMEM)] * len(terms),
        scratch_shapes=scratch,
        compiler_params=pltpu.CompilerParams(
            collective_id=1, has_side_effects=True, vmem_limit_bytes=67043328
        ),
        cost_estimate=pl.CostEstimate(
            flops=2_000_000_000, bytes_accessed=30_000_000, transcendentals=0
        ),
    )(*[term.reshape(4, 4, *shape) for term, shape in zip(terms, shapes)])
    return pl.pallas_call(
        hand_over,
        out_shape=[jax.ShapeDtypeStruct(shape, jnp.float32) for shape in shapes],
        in_specs=[pl.BlockSpec(memory_space=pltpu.VMEM)] * len(sums),
        out_specs=[pl.BlockSpec(memory_space=pl.ANY)] * len(sums),
        scratch_shapes=[pltpu.SemaphoreType.DMA((len(sums),))],
        compiler_params=pltpu.CompilerParams(vmem_limit_bytes=67043328),
    )(*sums)


def repeat(bound, body, unroll):
    def step(index, carry):
        body(index)
        return carry

    lax.fori_loop(0, bound, step, 0, unroll=unroll)


def cell_mask(cells, block):
    row = cells[pl.ds(block, 1), :]
    place = lax.broadcasted_iota(jnp.int32, (TILE, row.shape[1]), 0)
    return (jnp.broadcast_to(row, place.shape) == place).astype(jnp.bfloat16)


def deposit_kernel(slots, cells, features, out):
    zero = jnp.zeros((TILE, TILE), jnp.bfloat16)

    def clear(slot):
        out[slot] = zero

    repeat(out.shape[0], clear, 8)

    def deposit(block):
        value = jnp.dot(
            cell_mask(cells, block), features[block], preferred_element_type=jnp.float32
        )
        out[slots[block]] = value.astype(jnp.bfloat16)

    repeat(features.shape[0], deposit, 8)


def splat_kernel(tiles, incoming, base, out, canvas):
    zero = jnp.zeros((TILE, TILE), jnp.float32)

    def clear(tile):
        canvas[tile] = zero

    repeat(canvas.shape[0], clear, 3)

    def add(slot):
        tile = tiles[slot]
        canvas[tile] = canvas[tile] + incoming[slot].astype(jnp.float32)

    repeat(incoming.shape[0], add, 4)

    def finish(row):
        for k in range(4):
            for half in range(2):
                cells = slice(k * 64 + half * 32, k * 64 + half * 32 + 32)
                total = base[row, cells].astype(jnp.float32)
                total = total + canvas[2 * row + half, k * 32 : k * 32 + 32]
                out[row, cells] = total.astype(jnp.bfloat16)

    repeat(out.shape[0], finish, 2)


def pick_kernel(tiles, gradient, out):
    def pick(slot):
        tile = tiles[slot]
        row, half = lax.div(tile, 2), lax.rem(tile, 2)
        for k in range(4):
            cells = pl.ds(pl.multiple_of(k * 64 + half * 32, 32), 32)
            out[slot, k * 32 : k * 32 + 32] = gradient[row, cells]

    repeat(out.shape[0], pick, 4)


def camera_kernel(slots, cells, returned, out):
    def camera(block):
        out[block] = outer(cell_mask(cells, block), returned[slots[block]]).astype(jnp.bfloat16)

    repeat(out.shape[0], camera, 8)


def local_call(kernel, shape, operands, scratch=()):
    vector = pl.BlockSpec(memory_space=pltpu.VMEM)
    return pl.pallas_call(
        kernel,
        out_shape=jax.ShapeDtypeStruct(shape, jnp.bfloat16),
        in_specs=[pl.BlockSpec(memory_space=pltpu.SMEM)] + [vector] * (len(operands) - 1),
        out_specs=vector,
        scratch_shapes=scratch,
        compiler_params=pltpu.CompilerParams(vmem_limit_bytes=40000000),
        cost_estimate=pl.CostEstimate(
            flops=400_000_000, bytes_accessed=8_000_000, transcendentals=0
        ),
    )(*operands)


def by_parity(field):
    rows, across, channels = field.shape
    return (
        field.reshape(rows, across // 4, 2, 2, channels)
        .transpose(0, 3, 2, 1, 4)
        .reshape(rows, across, channels)
    )


def body(
    camera_features,
    cell_index,
    owner_device,
    owner_tile,
    base_map,
    targets,
    fine_conv,
    fine_down,
    middle_conv,
    middle_down,
    coarse_conv,
    coarse_up,
    middle_merge,
    middle_up,
    fine_merge,
    head_weight,
):
    single = jnp.float32
    bfloat = jnp.bfloat16
    device = lax.axis_index("slab")
    devices = lax.axis_size("slab")
    height, across, channels = base_map.shape
    slot_count = devices * CAP
    tile_count = height * across // TILE
    owners = owner_device[:, 0]
    everyone = owners.shape[0]
    choose = (owners[:, None] == jnp.arange(devices, dtype=jnp.int32)[None, :]).astype(jnp.int32)
    grouped = choose.reshape(devices, BLK_DEV, devices)
    earlier = (jnp.cumsum(grouped, axis=1) - grouped).reshape(everyone, devices)
    ranking = jnp.sum(earlier * choose, axis=1)
    sources = jnp.arange(everyone, dtype=jnp.int32) // BLK_DEV
    slot_number = owners * CAP + ranking
    local_slot = lax.dynamic_slice_in_dim(slot_number, device * BLK_DEV, BLK_DEV)
    slot_range = jnp.arange(slot_count, dtype=jnp.int32)
    arrival = sources * CAP + ranking
    receive_map = ((arrival[None, :] == slot_range[:, None]) & (owners[None, :] == device)).astype(
        jnp.int32
    )
    received = jnp.sum(receive_map, axis=1)
    slot_tiles = jnp.sum(receive_map * owner_tile[None, :], axis=1)
    landing_tiles = jnp.where(received > 0, slot_tiles, tile_count)
    local_cells = lax.dynamic_slice_in_dim(cell_index, device * BLK_DEV, BLK_DEV)
    local_cells = local_cells % 2 * 64 + local_cells // 2 % 2 * 32 + local_cells // 4
    wire = (devices, CAP * TILE, channels)
    outgoing = local_call(
        deposit_kernel,
        (slot_count, TILE, channels),
        (local_slot, local_cells, camera_features),
    )
    incoming = lax.all_to_all(
        outgoing.reshape(wire), "slab", split_axis=0, concat_axis=0, tiled=True
    ).reshape(slot_count, TILE, channels)
    level_zero = local_call(
        splat_kernel,
        (height, across, channels),
        (landing_tiles, incoming, by_parity(base_map)),
        [pltpu.VMEM((tile_count + 1, TILE, channels), single)],
    )
    level_zero_grad, losses, *terms = unet(
        level_zero,
        by_parity(targets),
        fine_conv,
        fine_down,
        middle_conv,
        middle_down,
        coarse_conv,
        coarse_up,
        middle_merge,
        middle_up,
        fine_merge,
        head_weight,
        flipped(fine_conv),
        flipped(middle_conv),
        flipped(coarse_conv),
        flipped(middle_merge),
        flipped(fine_merge),
    )
    row_loss = jnp.sum(losses[:, 0, :], axis=1) / (across * K)
    slot_grad = local_call(
        pick_kernel, (slot_count, TILE, channels), (slot_tiles, level_zero_grad)
    )
    returned = lax.all_to_all(
        slot_grad.reshape(wire), "slab", split_axis=0, concat_axis=0, tiled=True
    ).reshape(slot_count, TILE, channels)
    camera_grad = local_call(
        camera_kernel, camera_features.shape, (local_slot, local_cells, returned)
    )
    sums = scatter_sums(terms)
    return (camera_grad, row_loss, *sums)


def solution(mesh):
    step = jax.shard_map(
        body,
        mesh=mesh,
        in_specs=(
            P(("scene", "slab"), None, None),
            P("scene", None),
            P("scene", None),
            P("scene"),
            P(("scene", "slab"), None, None),
            P(("scene", "slab"), None, None),
            P(),
            P(),
            P(),
            P(),
            P(),
            P(),
            P(),
            P(),
            P(),
            P(),
        ),
        out_specs=(
            P(("scene", "slab"), None, None),
            P(("scene", "slab")),
            P(("scene", "slab"), None),
            P(("scene", "slab"), None),
            P(("scene", "slab"), None),
            P(("scene", "slab"), None),
            P(("scene", "slab"), None),
            P(("scene", "slab"), None),
            P(("scene", "slab"), None),
            P(("scene", "slab"), None),
            P(("scene", "slab"), None),
            P(("scene", "slab"), None),
        ),
        check_vma=False,
    )
    return step
```
